32 devices in a mesh: slab: 32 (over z, y, x, core).
Axes of the slice: x: 2, y: 2, z: 4, core: 2. Of those that a mesh axis runs over, the one named last changes fastest.
Arguments:
- load_terms: float32 [8, 8, 8, 4096], P(None, None, None, 'slab'), may hold values from -12 to 12
- geometry: float32 [3, 8, 8, 8, 4096], P(None, None, None, None, 'slab'), may hold values from 0.02 to 0.2
- mass_terms: float32 [8, 8, 8, 4096], P(None, None, None, 'slab'), may hold values from 1 to 4
- element_order: int32 [32, 128], P('slab'), may hold values from 0 to 127, each once within a row
Outputs:
- solution: float32 [8, 8, 8, 4096], P(None, None, None, 'slab')
- residual: float32 [8, 8, 8, 4096], P(None, None, None, 'slab')
The draws below stay inside these ranges and needn't reach their ends.
Inputs may be any that keep to these rules, and one draw needn't show every extreme that they name: `element_order`: each device's row lists each of its 128 cells once.
All inputs are finite; a program needn't handle non-finite values.
Results may differ from the reference program's by a relative error of at most 0.0001.
Values sent between devices are 32-bit elements; how exact they have to be, the bound alone decides.
A program may use at most 64 MiB of HBM per device.

```python
import math
import jax
import jax.numpy as jnp
import numpy as np
from jax import lax

POINTS = 8
EL_X = 1
EL_Y = 8
EL_Z = 16
SECTIONS = 2
ELEM_DEV = 128
NELEM = 4096
N_SLAB = 32


def draw_load_terms(key, part):
    noise = jax.random.normal(key, (POINTS, POINTS, POINTS, NELEM), jnp.float32)
    device_pos = (jnp.arange(NELEM) // ELEM_DEV).astype(jnp.float32)
    ramp = 1.0 + 0.8 * device_pos / max(NELEM // ELEM_DEV - 1, 1)
    return jnp.clip(noise * ramp, -12.0, 12.0)


def level_of(own_key, dims, split, smallest, high):
    level = 1.0
    for position, shards_of in split:
        steps = jax.random.uniform(jax.random.fold_in(jax.random.fold_in(own_key, 6), position), (shards_of,), jnp.float32, smallest / len(split), high / len(split))
        level = level * jnp.repeat(jnp.exp(steps), dims[position] // shards_of).reshape((-1,) + (1,) * (len(dims) - 1 - position))
    return level


def setup_inputs(seed: int = 0) -> dict:
    key_of = jax.random.split(jax.random.key(seed), 5)
    load_terms = draw_load_terms(jax.random.fold_in(key_of[4], 71), 0)
    geometry = jnp.clip(jnp.exp(math.log(0.2) - 2.3025851 * jax.random.uniform(key_of[1], (3, POINTS, POINTS, POINTS, NELEM), jnp.float32) ** level_of(key_of[1], (3, POINTS, POINTS, POINTS, NELEM), ((4, 32),), -0.2, 0.2)), 0.02, 0.2)
    mass_terms = jnp.clip(jnp.exp(math.log(4.0) - 1.3862944 * jax.random.uniform(key_of[2], (POINTS, POINTS, POINTS, NELEM), jnp.float32) ** level_of(key_of[2], (POINTS, POINTS, POINTS, NELEM), ((3, 32),), -0.2, 0.2)), 1.0, 4.0)
    element_order = jax.vmap(lambda own: jax.random.permutation(own, ELEM_DEV))(jax.random.split(key_of[3], N_SLAB)).reshape((N_SLAB, ELEM_DEV)).astype(jnp.int32)
    return dict(load_terms=load_terms, geometry=geometry, mass_terms=mass_terms, element_order=element_order)


spectrum_centre = 1.65
spectrum_half = 1.35


def legendre_table(positions, points):
    columns = [positions * 0.0 + 1.0, positions]
    for degree_now in range(2, points):
        columns.append(((2 * degree_now - 1) * positions * columns[-1] - (degree_now - 1) * columns[-2]) / degree_now)
    return np.stack(columns, axis=1)


def gll_derivative(points):
    degree = points - 1
    grid_nodes = -np.cos(np.pi * np.arange(points) / degree)
    for repeat in range(100):
        legendre = legendre_table(grid_nodes, points)
        grid_nodes = grid_nodes - (grid_nodes * legendre[:, degree] - legendre[:, degree - 1]) / (points * legendre[:, degree])
    legendre = legendre_table(grid_nodes, points)
    top_values = legendre[:, degree]
    index_list = np.arange(points)
    same_index = index_list[:, None] == index_list[None, :]
    spacing = grid_nodes[:, None] - grid_nodes[None, :]
    spacing = np.where(same_index, 1.0, spacing)
    deriv_table = top_values[:, None] / (top_values[None, :] * spacing)
    deriv_table = np.where(same_index, 0.0, deriv_table)
    deriv_table[0, 0] = -degree * points / 4.0
    deriv_table[degree, degree] = degree * points / 4.0
    return deriv_table


def local_apply(values, geometry, mass_terms, deriv_table):
    highest = lax.Precision.HIGHEST
    grad_one = jnp.einsum("ma,abce->mbce", deriv_table, values, precision=highest)
    result = jnp.einsum("ma,mbce->abce", deriv_table, geometry[0] * grad_one, precision=highest)
    grad_two = jnp.einsum("mb,abce->amce", deriv_table, values, precision=highest)
    result = result + jnp.einsum("mb,amce->abce", deriv_table, geometry[1] * grad_two, precision=highest)
    grad_three = jnp.einsum("mc,abce->abme", deriv_table, values, precision=highest)
    result = result + jnp.einsum("mc,abme->abce", deriv_table, geometry[2] * grad_three, precision=highest)
    return result + mass_terms * values


def local_diagonal(geometry, mass_terms, deriv_table):
    highest = lax.Precision.HIGHEST
    squared = deriv_table * deriv_table
    result = jnp.einsum("ma,mbce->abce", squared, geometry[0], precision=highest)
    result = result + jnp.einsum("mb,amce->abce", squared, geometry[1], precision=highest)
    result = result + jnp.einsum("mc,abme->abce", squared, geometry[2], precision=highest)
    return result + mass_terms


def to_grid(values, element_order):
    points = values.shape[0]
    inverse = jnp.argsort(element_order, axis=1).astype(jnp.int32)
    row_base = jnp.arange(N_SLAB, dtype=jnp.int32)[:, None] * ELEM_DEV
    picks = (row_base + inverse).reshape(-1).astype(jnp.int32)
    grid = jnp.take(values, picks, axis=3)
    return grid.reshape(points, points, points, N_SLAB * EL_X, EL_Y, EL_Z)


def to_store(grid, element_order):
    points = grid.shape[0]
    row_base = jnp.arange(N_SLAB, dtype=jnp.int32)[:, None] * ELEM_DEV
    picks = (row_base + element_order.astype(jnp.int32)).reshape(-1).astype(jnp.int32)
    return jnp.take(grid.reshape(points, points, points, NELEM), picks, axis=3)


def assemble_grid(grid):
    low_face = grid[0]
    high_face = grid[-1]
    shared = high_face + jnp.roll(low_face, -1, axis=2)
    grid = jnp.concatenate([jnp.roll(shared, 1, axis=2)[None], grid[1:-1], shared[None]], axis=0)
    low_face = grid[:, 0]
    high_face = grid[:, -1]
    zero_column = jnp.zeros_like(low_face[:, :, :, :1])
    new_high = high_face + jnp.concatenate([low_face[:, :, :, 1:], zero_column], axis=3)
    new_low = low_face + jnp.concatenate([zero_column, high_face[:, :, :, :-1]], axis=3)
    grid = jnp.concatenate([new_low[:, None], grid[:, 1:-1], new_high[:, None]], axis=1)
    low_face = grid[:, :, 0]
    high_face = grid[:, :, -1]
    shared = high_face + jnp.roll(low_face, -1, axis=4)
    grid = jnp.concatenate([jnp.roll(shared, 1, axis=4)[:, :, None], grid[:, :, 1:-1], shared[:, :, None]], axis=2)
    return grid


def grid_weights(points):
    node_ids = jnp.arange(points)
    end_node = (node_ids == 0) | (node_ids == points - 1)
    edge_mult = jnp.where(end_node, 2.0, 1.0).astype(jnp.float32)
    cross_ids = jnp.arange(EL_Y)
    low_shared = (node_ids == 0)[:, None] & (cross_ids > 0)[None, :]
    high_shared = (node_ids == points - 1)[:, None] & (cross_ids < EL_Y - 1)[None, :]
    mid_mult = jnp.where(low_shared | high_shared, 2.0, 1.0).astype(jnp.float32)
    total = edge_mult[:, None, None, None, None, None] * mid_mult[None, :, None, None, :, None] * edge_mult[None, None, :, None, None, None]
    full = jnp.broadcast_to(total, (points, points, points, N_SLAB * EL_X, EL_Y, EL_Z))
    return 1.0 / full


def reference(load_terms, geometry, mass_terms, element_order):
    points = load_terms.shape[0]
    deriv_table = jnp.asarray(gll_derivative(points), jnp.float32)

    def stiffness_sum(values):
        return to_store(assemble_grid(to_grid(values, element_order)), element_order)

    def operate(values):
        return stiffness_sum(local_apply(values, geometry, mass_terms, deriv_table))

    weight = to_store(grid_weights(points), element_order)
    start = stiffness_sum(load_terms)
    inv_diag = 1.0 / stiffness_sum(local_diagonal(geometry, mass_terms, deriv_table))
    ratio_sigma = spectrum_centre / spectrum_half
    step_vec = inv_diag * start / spectrum_centre
    precond = step_vec
    rho_prev = 1.0 / ratio_sigma
    for section in range(SECTIONS - 1):
        rho_next = 1.0 / (2.0 * ratio_sigma - rho_prev)
        misfit = start - operate(precond)
        step_vec = rho_next * rho_prev * step_vec + (2.0 * rho_next / spectrum_half) * inv_diag * misfit
        precond = precond + step_vec
        rho_prev = rho_next
    numerator = jnp.sum(weight * start * precond)
    image_vec = operate(precond)
    denominator = jnp.sum(weight * precond * image_vec)
    step_size = numerator / denominator
    return step_size * precond, start - step_size * image_vec
```

```python
import functools

import jax
import jax.numpy as jnp
import numpy as np
from jax import lax
from jax.experimental import pallas as pl
from jax.experimental.pallas import tpu as pltpu
from jax.sharding import PartitionSpec as P

EL_Y = 8
EL_Z = 16
MESH = pl.DeviceIdType.MESH
WIDEST = 32

spectrum_centre = 1.65
spectrum_half = 1.35


def legendre_table(positions, points):
    columns = [positions * 0.0 + 1.0, positions]
    for degree_now in range(2, points):
        columns.append(
            ((2 * degree_now - 1) * positions * columns[-1] - (degree_now - 1) * columns[-2])
            / degree_now
        )
    return np.stack(columns, axis=1)


def gll_derivative(points):
    degree = points - 1
    grid_nodes = -np.cos(np.pi * np.arange(points) / degree)
    for repeat in range(100):
        legendre = legendre_table(grid_nodes, points)
        grid_nodes = grid_nodes - (grid_nodes * legendre[:, degree] - legendre[:, degree - 1]) / (
            points * legendre[:, degree]
        )
    legendre = legendre_table(grid_nodes, points)
    top_values = legendre[:, degree]
    index_list = np.arange(points)
    same_index = index_list[:, None] == index_list[None, :]
    spacing = grid_nodes[:, None] - grid_nodes[None, :]
    spacing = np.where(same_index, 1.0, spacing)
    deriv_table = top_values[:, None] / (top_values[None, :] * spacing)
    deriv_table = np.where(same_index, 0.0, deriv_table)
    deriv_table[0, 0] = -degree * points / 4.0
    deriv_table[degree, degree] = degree * points / 4.0
    return deriv_table


def radices(count):
    factors = []
    while count > 1:
        width = max([w for w in range(2, WIDEST + 1) if count % w == 0], default=count)
        factors.append(width)
        count //= width
    return factors


def contract(values, table, symmetric, skip_in=0, skip_out=0):
    points = len(values)
    half = points // 2
    ins = range(skip_in, half)
    even = {j: values[j] + values[points - 1 - j] for j in ins}
    odd = {j: values[j] - values[points - 1 - j] for j in ins}
    low, high = [], []
    for m in range(skip_out, half):
        part_even, part_odd = None, None
        for j in ins:
            a = float(0.5 * (table[m, j] + table[m, points - 1 - j]))
            b = float(0.5 * (table[m, j] - table[m, points - 1 - j]))
            part_even = a * even[j] if part_even is None else part_even + a * even[j]
            part_odd = b * odd[j] if part_odd is None else part_odd + b * odd[j]
        low.append(part_even + part_odd)
        high.append(part_even - part_odd if symmetric else part_odd - part_even)
    return low + high[::-1]


def end_columns(values, deriv):
    points = len(values)
    half = points // 2
    even = [values[m] + values[points - 1 - m] for m in range(half)]
    odd = [values[m] - values[points - 1 - m] for m in range(half)]
    low, high = {}, {}
    for a in range(1, points - 1):
        product = deriv[:, 0] * deriv[:, a]
        part_even, part_odd = None, None
        for m in range(half):
            p = float(0.5 * (product[m] + product[points - 1 - m]))
            q = float(0.5 * (product[m] - product[points - 1 - m]))
            part_even = p * even[m] if part_even is None else part_even + p * even[m]
            part_odd = q * odd[m] if part_odd is None else part_odd + q * odd[m]
        low[a] = part_even + part_odd
        high[points - 1 - a] = part_even - part_odd
    product = deriv[:, 0] * deriv[:, points - 1]
    cross = float(product[0]) * even[0]
    for m in range(1, half):
        cross = cross + float(product[m]) * even[m]
    return low, high, cross


def sum_of(terms):
    while len(terms) > 1:
        terms = [x + y for x, y in zip(terms[::2], terms[1::2])] + terms[len(terms) & ~1:]
    return terms[0]


def lane_gather(values, columns):
    dims = lax.GatherDimensionNumbers(
        offset_dims=(),
        collapsed_slice_dims=(1,),
        start_index_map=(1,),
        operand_batching_dims=(0,),
        start_indices_batching_dims=(0,),
    )
    return lax.gather(
        values, columns[..., None], dims, (1, 1), mode=lax.GatherScatterMode.PROMISE_IN_BOUNDS
    )


def kernel(
    count, points, factors, deriv,
    load_hbm, geo_hbm, mass_hbm, order_hbm, start, vec, image, size_ref,
    load, geo, mass, inverse, work,
    first_out, first_in, pair_in, pair, pair_diag, face_diag,
    ends, cross, inner_part, along_out, along_in,
    own_inv, near_inv, across, order, coef, sums, *rest,
):
    parts_in = rest[: len(factors)]
    (
        in_sem, first_send, first_recv, inv_send, inv_recv, pair_send, pair_recv,
        along_send, along_recv, sum_send, sum_recv,
    ) = rest[len(factors):]
    me = lax.axis_index("slab")
    right = lax.rem(me + 1, count)
    left = lax.rem(me + count - 1, count)
    plane = points * points
    rows = points * plane
    last = rows - plane
    cols = load.shape[1]
    odd_one = lax.rem(me, 2)
    near = 1 - odd_one
    far = odd_one
    near_device = lax.rem(me + count + 1 - 2 * odd_one, count)
    far_device = lax.rem(me + count - 1 + 2 * odd_one, count)
    device_of = ((far, far_device), (near, near_device))

    fetch = [
        pltpu.make_async_copy(geo_hbm, geo, in_sem.at[0]),
        pltpu.make_async_copy(mass_hbm, mass, in_sem.at[1]),
        pltpu.make_async_copy(load_hbm, load, in_sem.at[2]),
        pltpu.make_async_copy(order_hbm, order, in_sem.at[3]),
    ]
    for copy in fetch[::-1][:1] + fetch[:3]:
        copy.start()

    def peer(stride, width, k):
        digit = lax.rem(me // stride, width)
        return me + (lax.rem(digit + k, width) - digit) * stride

    strides = [int(np.prod(factors[:i])) for i in range(len(factors))]
    barrier = pltpu.get_barrier_semaphore()
    for beside in (left, right):
        pl.semaphore_signal(barrier, inc=1, device_id=(beside,), device_id_type=MESH)
    for stride, width in zip(strides, factors):
        @pl.loop(1, width)
        def _(k):
            pl.semaphore_signal(
                barrier, inc=1, device_id=(peer(stride, width, k),), device_id_type=MESH
            )

    fetch[3].wait()
    cell = order[...]
    cell8 = jnp.broadcast_to(cell, (points, cols))
    cell_col = jnp.transpose(jnp.broadcast_to(cell.astype(jnp.float32), (cols, cols)))
    lane = lax.broadcasted_iota(jnp.int32, (cols, cols), 1).astype(jnp.float32)
    source = lax.broadcasted_iota(jnp.int32, (cols, cols), 0).astype(jnp.float32)
    inv_row = jnp.sum(jnp.where(cell_col == lane, source, 0.0), axis=0, keepdims=True)
    inv8 = jnp.broadcast_to(inv_row.astype(jnp.int32), (points, cols))
    own_inv[...] = inv8
    pos_z = cell8 % EL_Z
    has_up = cell8 < cols - EL_Z
    has_down = cell8 >= EL_Z
    plus_y = lane_gather(inv8, jnp.where(has_up, cell8 + EL_Z, cell8))
    minus_y = lane_gather(inv8, jnp.where(has_down, cell8 - EL_Z, cell8))
    plus_z = lane_gather(inv8, jnp.where(pos_z == EL_Z - 1, cell8 - (EL_Z - 1), cell8 + 1))
    minus_z = lane_gather(inv8, jnp.where(pos_z == 0, cell8 + (EL_Z - 1), cell8 - 1))

    row_id = lax.broadcasted_iota(jnp.int32, (points, cols), 0)
    for t, table in enumerate((deriv, deriv.T, (deriv * deriv).T)):
        for k in range(points):
            vector = jnp.zeros((points, cols), jnp.float32)
            for m in range(points):
                vector = jnp.where(row_id == m, float(table[m, (m - k) % points]), vector)
            coef[t, k] = vector
    share_z = jnp.where((row_id == 0) | (row_id == points - 1), 0.5, 1.0)
    share_low = jnp.where(has_down, 0.5 * share_z, share_z)
    share_high = jnp.where(has_up, 0.5 * share_z, share_z)

    def share(b):
        return share_low if b == 0 else share_high if b == points - 1 else share_z

    def rotate_contract(value, t):
        total = coef[t, 0] * value
        for k in range(1, points):
            total = total + coef[t, k] * pltpu.roll(value, k, 0)
        return total

    def post(src, dst, send_sem, recv_sem, device):
        pltpu.make_async_remote_copy(
            src_ref=src, dst_ref=dst, send_sem=send_sem, recv_sem=recv_sem,
            device_id=(device,), device_id_type=MESH,
        ).start()

    def settle(ref, send_sem, recv_sem):
        return pltpu.make_async_remote_copy(
            src_ref=ref, dst_ref=ref, send_sem=send_sem, recv_sem=recv_sem,
            device_id=(right,), device_id_type=MESH,
        )

    def line(b):
        return pl.ds(b * points, points)

    def at(base, b):
        if isinstance(base, int):
            return pl.ds(base + b * points, points)
        return pl.ds(pl.multiple_of(base + b * points, points), points)

    def geo_at(k, base, b):
        return at(k * rows + base, b)

    def end_base(s):
        return pl.multiple_of(s * last, points)

    inner = [a * plane for a in range(1, points - 1)]

    def assemble_planes(spots):
        lows = [ref[at(base, 0)] for ref, base in spots]
        highs = [ref[at(base, points - 1)] for ref, base in spots]
        from_low = [lane_gather(low, plus_y) for low in lows]
        from_high = [lane_gather(high, minus_y) for high in highs]
        for i, (ref, base) in enumerate(spots):
            ref[at(base, points - 1)] = highs[i] + jnp.where(has_up, from_low[i], 0.0)
            ref[at(base, 0)] = lows[i] + jnp.where(has_down, from_high[i], 0.0)
        firsts = [pl.ds(base, points, stride=points) for _, base in spots]
        ends_at = [pl.ds(base + points - 1, points, stride=points) for _, base in spots]
        lows = [ref[first] for (ref, _), first in zip(spots, firsts)]
        highs = [ref[end] for (ref, _), end in zip(spots, ends_at)]
        from_low = [lane_gather(low, plus_z) for low in lows]
        from_high = [lane_gather(high, minus_z) for high in highs]
        for i, (ref, _) in enumerate(spots):
            ref[ends_at[i]] = highs[i] + from_low[i]
            ref[firsts[i]] = lows[i] + from_high[i]

    square = deriv * deriv
    fetch[0].wait()
    fetch[1].wait()

    for b in range(points):
        values = [geo[geo_at(0, a * plane, b)] for a in range(points)]
        for a, value in enumerate(contract(values, square.T, True)):
            work[at(a * plane, b)] = value

    def diagonal_plane(base, put):
        values = [geo[geo_at(1, base, b)] for b in range(points)]
        for b, value in enumerate(contract(values, square.T, True)):
            value = value + rotate_contract(geo[geo_at(2, base, b)], 2)
            put(b, value + work[at(base, b)] + mass[at(base, b)])

    for s, base in ((0, 0), (1, last)):

        def put(b, value):
            first_out[s, at(plane, b)] = value

        diagonal_plane(base, put)
    fetch[2].wait()
    for s, base in ((0, 0), (1, last)):
        for b in range(points):
            first_out[s, line(b)] = load[at(base, b)]
    assemble_planes([(first_out.at[s], k * plane) for s in (0, 1) for k in (0, 1)])

    for base in inner:
        for b in range(points):
            start[at(base, b)] = load[at(base, b)]

        def put(b, value):
            inverse[at(base, b)] = value

        diagonal_plane(base, put)
    assemble_planes([(ref, base) for base in inner for ref in (start, inverse)])
    for base in inner:
        for b in range(points):
            span = at(base, b)
            scaled = 1.0 / inverse[span]
            inverse[span] = scaled
            vec[span] = scaled * start[span] * (1.0 / spectrum_centre)
    for b in range(points):
        values = [geo[geo_at(0, a * plane, b)] for a in range(points)]
        low, high, both = end_columns(values, deriv)
        for a in range(1, points - 1):
            ends[0, at((a - 1) * plane, b)] = low[a]
            ends[1, at((a - 1) * plane, b)] = high[a]
        cross[line(b)] = both
    assemble_planes(
        [(ends.at[s], base - plane) for s in (0, 1) for base in inner] + [(cross, 0)]
    )

    def inner_to_ends():
        for b in range(points):
            values = [vec[at(base, b)] for base in inner]
            for s in (0, 1):
                inner_part[s, line(b)] = sum_of(
                    [ends[s, at(base - plane, b)] * v for base, v in zip(inner, values)]
                )

    inner_to_ends()

    pl.semaphore_wait(barrier, 2 + sum(w - 1 for w in factors))
    for s, device in device_of:
        post(first_out.at[s], first_in.at[1 - s], first_send, first_recv.at[1 - s], device)
        post(own_inv, near_inv.at[1 - s], inv_send, inv_recv.at[1 - s], device)
    for s, device in device_of:
        for k in (1, 2):
            post(
                geo.at[pl.ds(pl.multiple_of(k * rows + s * last, points), plane)],
                pair_in.at[1 - s, k - 1], pair_send, pair_recv.at[1 - s], device,
            )

    def in_plane(values, slope_geo, flux_geo):
        slopes = contract(values, deriv, False)
        fluxes = [slope_geo(b) * slopes[b] for b in range(points)]
        out = contract(fluxes, deriv.T, False)
        for b in range(points):
            flux = flux_geo(b) * rotate_contract(values[b], 0)
            out[b] = out[b] + rotate_contract(flux, 1)
        return out

    def apply_inner(extra):
        for b in range(points):
            values = [None] + [vec[at(base, b)] for base in inner] + [None]
            slopes = contract(values, deriv, False, skip_in=1)
            fluxes = [geo[geo_at(0, a * plane, b)] * slopes[a] for a in range(points)]
            terms = contract(fluxes, deriv.T, False, skip_out=1)
            for base, value in zip(inner, terms):
                work[at(base, b)] = value
        for base in inner:
            values = [vec[at(base, b)] for b in range(points)]
            terms = in_plane(
                values,
                lambda b: geo[geo_at(1, base, b)],
                lambda b: geo[geo_at(2, base, b)],
            )
            for b in range(points):
                span = at(base, b)
                out = terms[b] + work[span] + mass[span] * values[b]
                image[span] = out
                extra(span, values[b], out)

    apply_inner(lambda span, value, out: None)
    assemble_planes([(image, base) for base in inner])

    def meet(s):
        settle(near_inv.at[s], inv_send, inv_recv.at[s]).wait_recv()
        columns = lane_gather(near_inv[s], cell8)
        across[s] = columns
        settle(first_in.at[s], first_send, first_recv.at[s]).wait_recv()
        base = end_base(s)
        for b in range(points):
            span = at(base, b)
            begin = first_out[s, line(b)] + lane_gather(first_in[s, line(b)], columns)
            whole = first_out[s, at(plane, b)] + lane_gather(first_in[s, at(plane, b)], columns)
            scaled = 1.0 / whole
            face_diag[s, line(b)] = whole
            start[span] = begin
            inverse[span] = scaled
            vec[span] = scaled * begin * (1.0 / spectrum_centre)

    def send_along(e, s, other, device):
        base = end_base(other)
        for b in range(points):
            along_out[e, s, line(b)] = inner_part[s, line(b)] + cross[line(b)] * vec[at(base, b)]
        post(
            along_out.at[e, s], along_in.at[e, 1 - s], along_send.at[e],
            along_recv.at[e, 1 - s], device,
        )

    def join_pair(s):
        settle(pair_in.at[s], pair_send, pair_recv.at[s]).wait_recv()
        columns = across[s]
        for k in (0, 1):
            for b in range(points):
                own = geo[geo_at(k + 1, s * last, b)]
                pair[s, k, line(b)] = own + lane_gather(pair_in[s, k, line(b)], columns)
        terms = contract([pair[s, 0, line(b)] for b in range(points)], square.T, True)
        for b in range(points):
            pair_diag[s, line(b)] = terms[b] + rotate_contract(pair[s, 1, line(b)], 2)

    def apply_end(s, ref):
        base = end_base(s)
        values = [vec[at(base, b)] for b in range(points)]
        terms = in_plane(values, lambda b: pair[s, 0, line(b)], lambda b: pair[s, 1, line(b)])
        for b in range(points):
            terms[b] = terms[b] - pair_diag[s, line(b)] * values[b]
            ref[at(base, b)] = terms[b]
        return values, terms

    def first_end(s):
        apply_end(s, image)
        assemble_planes([(image, end_base(s))])

    ratio_sigma = spectrum_centre / spectrum_half
    rho_prev = 1.0 / ratio_sigma
    rho_next = 1.0 / (2.0 * ratio_sigma - rho_prev)
    on_misfit = 2.0 * rho_next / spectrum_half
    on_start = (1.0 + rho_next * rho_prev) / spectrum_centre + on_misfit

    def add_ends(base, b):
        return (
            image[at(base, b)]
            + ends[0, at(base - plane, b)] * vec[at(0, b)]
            + ends[1, at(base - plane, b)] * vec[at(last, b)]
        )

    def join_along(e, s, columns, b):
        span = at(end_base(s), b)
        return (
            image[span] + face_diag[s, line(b)] * vec[span] + along_out[e, s, line(b)]
            + lane_gather(along_in[e, s, line(b)], columns)
        )

    def second_end(s):
        settle(along_in.at[0, s], along_send.at[0], along_recv.at[0, s]).wait_recv()
        columns = across[s]
        for b in range(points):
            span = at(end_base(s), b)
            total = join_along(0, s, columns, b)
            vec[span] = inverse[span] * (on_start * start[span] - on_misfit * total)

    on_load, products = [], []

    def end_terms(s):
        values, terms = apply_end(s, image)
        for b in range(points):
            value = values[b]
            halved = 0.5 * value
            weighted = share(b) * value
            span = at(end_base(s), b)
            on_load.append(0.5 * weighted * start[span])
            products.append(
                halved * terms[b]
                + weighted * (face_diag[s, line(b)] * halved + 2.0 * inner_part[s, line(b)])
            )

    meet(near)
    send_along(0, far, near, far_device)
    join_pair(near)
    first_end(near)
    meet(far)
    send_along(0, near, far, near_device)
    for base in inner:
        for b in range(points):
            span = at(base, b)
            total = add_ends(base, b)
            vec[span] = inverse[span] * (on_start * start[span] - on_misfit * total)
    join_pair(far)
    first_end(far)
    inner_to_ends()
    second_end(near)
    send_along(1, far, near, far_device)

    def tally(span, value, out):
        products.append(value * out)
        on_load.append(load[span] * value)

    apply_inner(tally)
    end_terms(near)
    second_end(far)
    send_along(1, near, far, near_device)
    end_terms(far)
    for b in range(points):
        products.append(
            2.0 * share(b) * cross[line(b)] * vec[at(0, b)] * vec[at(last, b)]
        )
    total = jnp.concatenate(
        [jnp.sum(sum_of(part), axis=0, keepdims=True) for part in (on_load, products)], axis=1
    )

    def sum_copy(i, k):
        stride, width = strides[i], factors[i]
        return pltpu.make_async_remote_copy(
            src_ref=sums.at[i], dst_ref=parts_in[i].at[k - 1],
            send_sem=sum_send.at[i], recv_sem=sum_recv.at[i],
            device_id=(peer(stride, width, k),), device_id_type=MESH,
        )

    def start_sum(i, value):
        sums[i] = value

        @pl.loop(1, factors[i])
        def _(k):
            sum_copy(i, k).start()

    def finish_sum(i, value):
        settle(parts_in[i], sum_send.at[i], sum_recv.at[i]).wait()
        for k in range(factors[i] - 1):
            value = value + parts_in[i][k]
        return value

    start_sum(0, total)

    assemble_planes([(image, base) for base in [0] + inner + [last]])
    for base in inner:
        for b in range(points):
            image[at(base, b)] = add_ends(base, b)
    for s in (near, far):
        settle(along_in.at[1, s], along_send.at[1], along_recv.at[1, s]).wait_recv()
        columns = across[s]
        for b in range(points):
            image[at(end_base(s), b)] = join_along(1, s, columns, b)
    settle(first_out, first_send, first_recv.at[0]).wait_send()
    settle(near_inv, inv_send, inv_recv.at[0]).wait_send()
    settle(pair_in, pair_send, pair_recv.at[0]).wait_send()
    for e in (0, 1):
        settle(along_out.at[e], along_send.at[e], along_recv.at[0, 0]).wait_send()
    for i in range(len(factors)):
        if i:
            start_sum(i, total)
        total = finish_sum(i, total)
    numerator = jnp.sum(total[:, :cols], axis=1, keepdims=True)
    denominator = jnp.sum(total[:, cols:], axis=1, keepdims=True)
    size_ref[...] = jnp.broadcast_to(numerator / denominator, (points, cols))


def finish(pieces, points, start, vec, image, size, sol_hbm, res_hbm, sol, res, sems):
    rows, cols = start.shape
    scale = size[...]
    step = rows // pieces
    copies = []
    for i in range(pieces):
        part = pl.ds(i * step, step)
        for j in range(step // points):
            span = pl.ds(i * step + j * points, points)
            sol[span] = scale * vec[span]
            res[span] = start[span] - scale * image[span]
        for k, (src, dst) in enumerate(((sol, sol_hbm), (res, res_hbm))):
            copy = pltpu.make_async_copy(src.at[part], dst.at[part], sems.at[k, i])
            copy.start()
            copies.append(copy)
    for copy in copies:
        copy.wait()


PIECES = 2


def on_device(count, load_terms, geometry, mass_terms, element_order):
    points = load_terms.shape[0]
    cols = load_terms.shape[3]
    plane = points * points
    rows = points * plane
    deriv = gll_derivative(points)
    factors = radices(count)
    f32 = jnp.float32

    def room(*shape, dtype=f32):
        return pltpu.VMEM(shape + (cols,), dtype)

    dma = pltpu.SemaphoreType.DMA
    scratch = (
        [room(rows), room(3 * rows), room(rows), room(rows), room(rows)]
        + [
            room(2, 2 * plane), room(2, 2 * plane), room(2, 2, plane), room(2, 2, plane),
            room(2, plane), room(2, plane),
            room(2, rows - 2 * plane), room(plane), room(2, plane),
            room(2, 2, plane), room(2, 2, plane),
            room(points, dtype=jnp.int32), room(2, points, dtype=jnp.int32),
            room(2, points, dtype=jnp.int32), room(1, dtype=jnp.int32),
            room(3, points, points),
            pltpu.VMEM((len(factors), 1, 2 * cols), f32),
        ]
        + [pltpu.VMEM((w - 1, 1, 2 * cols), f32) for w in factors]
        + [
            dma((4,)), dma, dma((2,)), dma, dma((2,)), dma, dma((2,)),
            dma((2,)), dma((2, 2)), dma((len(factors),)), dma((len(factors),)),
        ]
    )
    hbm = pl.BlockSpec(memory_space=pl.ANY)
    vmem = pl.BlockSpec(memory_space=pltpu.VMEM)
    pieces = pl.pallas_call(
        functools.partial(kernel, count, points, factors, deriv),
        out_shape=(pltpu.VMEM((rows, cols), f32),) * 3 + (pltpu.VMEM((points, cols), f32),),
        in_specs=[hbm] * 4,
        out_specs=(vmem,) * 4,
        scratch_shapes=scratch,
        compiler_params=pltpu.CompilerParams(collective_id=0, has_side_effects=True),
    )(
        load_terms.reshape(rows, cols),
        geometry.reshape(3 * rows, cols),
        mass_terms.reshape(rows, cols),
        element_order,
    )
    solution_rows, residual_rows = pl.pallas_call(
        functools.partial(finish, PIECES, points),
        out_shape=(jax.ShapeDtypeStruct((rows, cols), f32),) * 2,
        in_specs=[vmem] * 4,
        out_specs=(hbm, hbm),
        scratch_shapes=[room(rows), room(rows), dma((2, PIECES))],
        compiler_params=pltpu.CompilerParams(vmem_limit_bytes=8 * rows * cols * 4),
    )(*pieces)
    shape = load_terms.shape
    return solution_rows.reshape(shape), residual_rows.reshape(shape)


def solution(mesh):
    placed = (
        P(None, None, None, "slab"),
        P(None, None, None, None, "slab"),
        P(None, None, None, "slab"),
        P("slab", None),
    )
    return jax.shard_map(
        functools.partial(on_device, mesh.shape["slab"]),
        mesh=mesh,
        in_specs=placed,
        out_specs=(P(None, None, None, "slab"), P(None, None, None, "slab")),
        check_vma=False,
    )
```

```python
import functools

import jax
import jax.numpy as jnp
import numpy as np
from jax import lax
from jax.experimental import pallas as pl
from jax.experimental.pallas import tpu as pltpu
from jax.sharding import PartitionSpec as P

EL_Y = 8
EL_Z = 16
MESH = pl.DeviceIdType.MESH
WIDEST = 32
HALVES = 2

spectrum_centre = 1.65
spectrum_half = 1.35


def legendre_table(positions, points):
    columns = [positions * 0.0 + 1.0, positions]
    for degree_now in range(2, points):
        columns.append(
            ((2 * degree_now - 1) * positions * columns[-1] - (degree_now - 1) * columns[-2])
            / degree_now
        )
    return np.stack(columns, axis=1)


def gll_derivative(points):
    degree = points - 1
    grid_nodes = -np.cos(np.pi * np.arange(points) / degree)
    for repeat in range(100):
        legendre = legendre_table(grid_nodes, points)
        grid_nodes = grid_nodes - (grid_nodes * legendre[:, degree] - legendre[:, degree - 1]) / (
            points * legendre[:, degree]
        )
    legendre = legendre_table(grid_nodes, points)
    top_values = legendre[:, degree]
    index_list = np.arange(points)
    same_index = index_list[:, None] == index_list[None, :]
    spacing = grid_nodes[:, None] - grid_nodes[None, :]
    spacing = np.where(same_index, 1.0, spacing)
    deriv_table = top_values[:, None] / (top_values[None, :] * spacing)
    deriv_table = np.where(same_index, 0.0, deriv_table)
    deriv_table[0, 0] = -degree * points / 4.0
    deriv_table[degree, degree] = degree * points / 4.0
    return deriv_table


def radices(count):
    factors = []
    while count > 1:
        width = max([w for w in range(2, WIDEST + 1) if count % w == 0], default=count)
        factors.append(width)
        count //= width
    return factors


def square_split(width):
    return min(d for d in range(1, width + 1) if width % d == 0 and d * d >= width)


def contract(values, table, symmetric, skip_in=0, skip_out=0):
    points = len(values)
    half = points // 2
    ins = range(skip_in, half)
    even = {j: values[j] + values[points - 1 - j] for j in ins}
    odd = {j: values[j] - values[points - 1 - j] for j in ins}
    low, high = [], []
    for m in range(skip_out, half):
        part_even, part_odd = None, None
        for j in ins:
            a = float(0.5 * (table[m, j] + table[m, points - 1 - j]))
            b = float(0.5 * (table[m, j] - table[m, points - 1 - j]))
            part_even = a * even[j] if part_even is None else part_even + a * even[j]
            part_odd = b * odd[j] if part_odd is None else part_odd + b * odd[j]
        low.append(part_even + part_odd)
        high.append(part_even - part_odd if symmetric else part_odd - part_even)
    return low + high[::-1]


def end_columns(values, deriv):
    points = len(values)
    half = points // 2
    even = [values[m] + values[points - 1 - m] for m in range(half)]
    odd = [values[m] - values[points - 1 - m] for m in range(half)]
    low, high = {}, {}
    for a in range(1, points - 1):
        product = deriv[:, 0] * deriv[:, a]
        part_even, part_odd = None, None
        for m in range(half):
            p = float(0.5 * (product[m] + product[points - 1 - m]))
            q = float(0.5 * (product[m] - product[points - 1 - m]))
            part_even = p * even[m] if part_even is None else part_even + p * even[m]
            part_odd = q * odd[m] if part_odd is None else part_odd + q * odd[m]
        low[a] = part_even + part_odd
        high[points - 1 - a] = part_even - part_odd
    product = deriv[:, 0] * deriv[:, points - 1]
    cross = float(product[0]) * even[0]
    for m in range(1, half):
        cross = cross + float(product[m]) * even[m]
    return low, high, cross


def sum_of(terms):
    while len(terms) > 1:
        terms = [x + y for x, y in zip(terms[::2], terms[1::2])] + terms[len(terms) & ~1:]
    return terms[0]


def lane_gather(values, columns):
    dims = lax.GatherDimensionNumbers(
        offset_dims=(),
        collapsed_slice_dims=(1,),
        start_index_map=(1,),
        operand_batching_dims=(0,),
        start_indices_batching_dims=(0,),
    )
    return lax.gather(
        values, columns[..., None], dims, (1, 1), mode=lax.GatherScatterMode.PROMISE_IN_BOUNDS
    )


def kernel(
    count, points, factors, deriv,
    load_hbm, geo_hbm, mass_hbm, order_hbm, start, vec, image, size_ref,
    load, geo, mass, inverse, work,
    first_out, first_in, pair_in, pair, pair_diag, face_diag,
    ends, cross, inner_part, along_out, along_in,
    own_inv, near_inv, across, order, coef, sums, *rest,
):
    parts_in = rest[: len(factors)]
    (
        in_sem, first_send, first_recv, inv_send, inv_recv, pair_send, pair_recv,
        along_send, along_recv, sum_send, sum_recv, ready,
    ) = rest[len(factors):]
    me = lax.axis_index("slab")
    right = lax.rem(me + 1, count)
    left = lax.rem(me + count - 1, count)
    plane = points * points
    rows = points * plane
    last = rows - plane
    piece = plane // HALVES
    cols = load.shape[1]
    odd_one = lax.rem(me, 2)
    near = 1 - odd_one
    far = odd_one
    near_device = lax.rem(me + count + 1 - 2 * odd_one, count)
    far_device = lax.rem(me + count - 1 + 2 * odd_one, count)
    long_way = lax.rem((me + 1) // 2, 2) == 0

    fetch = [
        pltpu.make_async_copy(geo_hbm, geo, in_sem.at[0]),
        pltpu.make_async_copy(mass_hbm, mass, in_sem.at[1]),
        pltpu.make_async_copy(load_hbm, load, in_sem.at[2]),
        pltpu.make_async_copy(order_hbm, order, in_sem.at[3]),
    ]
    for copy in fetch[::-1][:1] + fetch[:3]:
        copy.start()

    def peer(stride, width, k):
        digit = lax.rem(me // stride, width)
        return me + (lax.rem(digit + k, width) - digit) * stride

    strides = [int(np.prod(factors[:i])) for i in range(len(factors))]
    barrier = pltpu.get_barrier_semaphore()
    for beside in (left, right):
        pl.semaphore_signal(barrier, inc=1, device_id=(beside,), device_id_type=MESH)
    blocks = [(stride, square_split(width)) for stride, width in zip(strides, factors)]
    columns_of = [
        (stride * size, width // size) for (stride, size), width in zip(blocks, factors)
    ]

    def greet(semaphore, groups):
        for stride, width in groups:
            @pl.loop(1, width)
            def _(k):
                pl.semaphore_signal(
                    semaphore, inc=1, device_id=(peer(stride, width, k),), device_id_type=MESH
                )

    greet(barrier, blocks + columns_of)

    fetch[3].wait()
    cell = order[...]
    cell8 = jnp.broadcast_to(cell, (points, cols))
    cell_col = jnp.transpose(jnp.broadcast_to(cell.astype(jnp.float32), (cols, cols)))
    lane = lax.broadcasted_iota(jnp.int32, (cols, cols), 1).astype(jnp.float32)
    source = lax.broadcasted_iota(jnp.int32, (cols, cols), 0).astype(jnp.float32)
    inv_row = jnp.sum(jnp.where(cell_col == lane, source, 0.0), axis=0, keepdims=True)
    inv8 = jnp.broadcast_to(inv_row.astype(jnp.int32), (points, cols))
    own_inv[...] = inv8
    pos_z = cell8 % EL_Z
    has_up = cell8 < cols - EL_Z
    has_down = cell8 >= EL_Z
    plus_y = lane_gather(inv8, jnp.where(has_up, cell8 + EL_Z, cell8))
    minus_y = lane_gather(inv8, jnp.where(has_down, cell8 - EL_Z, cell8))
    plus_z = lane_gather(inv8, jnp.where(pos_z == EL_Z - 1, cell8 - (EL_Z - 1), cell8 + 1))
    minus_z = lane_gather(inv8, jnp.where(pos_z == 0, cell8 + (EL_Z - 1), cell8 - 1))

    row_id = lax.broadcasted_iota(jnp.int32, (points, cols), 0)
    for t, table in enumerate((deriv, deriv.T, (deriv * deriv).T)):
        for k in range(points):
            vector = jnp.zeros((points, cols), jnp.float32)
            for m in range(points):
                vector = jnp.where(row_id == m, float(table[m, (m - k) % points]), vector)
            coef[t, k] = vector
    share_z = jnp.where((row_id == 0) | (row_id == points - 1), 0.5, 1.0)
    share_low = jnp.where(has_down, 0.5 * share_z, share_z)
    share_high = jnp.where(has_up, 0.5 * share_z, share_z)

    def share(b):
        return share_low if b == 0 else share_high if b == points - 1 else share_z

    def rotate_contract(value, t):
        total = coef[t, 0] * value
        for k in range(1, points):
            total = total + coef[t, k] * pltpu.roll(value, k, 0)
        return total

    def post(src, dst, send_sem, recv_sem, device):
        pltpu.make_async_remote_copy(
            src_ref=src, dst_ref=dst, send_sem=send_sem, recv_sem=recv_sem,
            device_id=(device,), device_id_type=MESH,
        ).start()

    def settle(ref, send_sem, recv_sem):
        return pltpu.make_async_remote_copy(
            src_ref=ref, dst_ref=ref, send_sem=send_sem, recv_sem=recv_sem,
            device_id=(right,), device_id_type=MESH,
        )

    def line(b):
        return pl.ds(b * points, points)

    def at(base, b):
        if isinstance(base, int):
            return pl.ds(base + b * points, points)
        return pl.ds(pl.multiple_of(base + b * points, points), points)

    def geo_at(k, base, b):
        return at(k * rows + base, b)

    def end_base(s):
        return pl.multiple_of(s * last, points)

    inner = [a * plane for a in range(1, points - 1)]

    def assemble_planes(spots):
        lows = [ref[at(base, 0)] for ref, base in spots]
        highs = [ref[at(base, points - 1)] for ref, base in spots]
        from_low = [lane_gather(low, plus_y) for low in lows]
        from_high = [lane_gather(high, minus_y) for high in highs]
        for i, (ref, base) in enumerate(spots):
            ref[at(base, points - 1)] = highs[i] + jnp.where(has_up, from_low[i], 0.0)
            ref[at(base, 0)] = lows[i] + jnp.where(has_down, from_high[i], 0.0)
        firsts = [pl.ds(base, points, stride=points) for _, base in spots]
        ends_at = [pl.ds(base + points - 1, points, stride=points) for _, base in spots]
        lows = [ref[first] for (ref, _), first in zip(spots, firsts)]
        highs = [ref[end] for (ref, _), end in zip(spots, ends_at)]
        from_low = [lane_gather(low, plus_z) for low in lows]
        from_high = [lane_gather(high, minus_z) for high in highs]
        for i, (ref, _) in enumerate(spots):
            ref[ends_at[i]] = highs[i] + from_low[i]
            ref[firsts[i]] = lows[i] + from_high[i]

    square = deriv * deriv
    fetch[0].wait()
    fetch[1].wait()

    for b in range(points):
        values = [geo[geo_at(0, a * plane, b)] for a in range(points)]
        for a, value in enumerate(contract(values, square.T, True)):
            work[at(a * plane, b)] = value

    def diagonal_plane(base, put):
        values = [geo[geo_at(1, base, b)] for b in range(points)]
        for b, value in enumerate(contract(values, square.T, True)):
            value = value + rotate_contract(geo[geo_at(2, base, b)], 2)
            put(b, value + work[at(base, b)] + mass[at(base, b)])

    for s, base in ((0, 0), (1, last)):

        def put(b, value):
            first_out[s, at(plane, b)] = value

        diagonal_plane(base, put)
    fetch[2].wait()
    for s, base in ((0, 0), (1, last)):
        for b in range(points):
            first_out[s, line(b)] = load[at(base, b)]
    assemble_planes([(first_out.at[s], k * plane) for s in (0, 1) for k in (0, 1)])

    for base in inner:
        for b in range(points):
            start[at(base, b)] = load[at(base, b)]

        def put(b, value):
            inverse[at(base, b)] = value

        diagonal_plane(base, put)
    assemble_planes([(ref, base) for base in inner for ref in (start, inverse)])
    for base in inner:
        for b in range(points):
            span = at(base, b)
            scaled = 1.0 / inverse[span]
            inverse[span] = scaled
            vec[span] = scaled * start[span] * (1.0 / spectrum_centre)
    for b in range(points):
        values = [geo[geo_at(0, a * plane, b)] for a in range(points)]
        low, high, both = end_columns(values, deriv)
        for a in range(1, points - 1):
            ends[0, at((a - 1) * plane, b)] = low[a]
            ends[1, at((a - 1) * plane, b)] = high[a]
        cross[line(b)] = both
    assemble_planes(
        [(ends.at[s], base - plane) for s in (0, 1) for base in inner] + [(cross, 0)]
    )

    def inner_to_ends(e, b, values):
        for s in (0, 1):
            inner_part[e, s, line(b)] = sum_of(
                [ends[s, at(base - plane, b)] * v for base, v in zip(inner, values)]
            )

    for b in range(points):
        inner_to_ends(0, b, [vec[at(base, b)] for base in inner])

    pl.semaphore_wait(barrier, 2 + sum(w - 1 for _, w in blocks + columns_of))

    def send_first(s, device):
        post(own_inv, near_inv.at[1 - s], inv_send, inv_recv.at[1 - s], device)
        for h in range(HALVES):
            for k in (0, 1):
                part = pl.ds(k * plane + h * piece, piece)
                post(
                    first_out.at[s, part], first_in.at[1 - s, part], first_send,
                    first_recv.at[1 - s, h], device,
                )

    def send_pair(s, device):
        for k in (1, 2):
            post(
                geo.at[pl.ds(pl.multiple_of(k * rows + s * last, points), plane)],
                pair_in.at[1 - s, k - 1], pair_send, pair_recv.at[1 - s], device,
            )

    send_first(far, far_device)

    @pl.when(long_way)
    def _():
        send_pair(far, far_device)

    send_first(near, near_device)
    send_pair(near, near_device)
    greet(ready, blocks)

    def in_plane(values, slope_geo, flux_geo):
        slopes = contract(values, deriv, False)
        fluxes = [slope_geo(b) * slopes[b] for b in range(points)]
        out = contract(fluxes, deriv.T, False)
        for b in range(points):
            flux = flux_geo(b) * rotate_contract(values[b], 0)
            out[b] = out[b] + rotate_contract(flux, 1)
        return out

    def apply_inner():
        for b in range(points):
            values = [None] + [vec[at(base, b)] for base in inner] + [None]
            slopes = contract(values, deriv, False, skip_in=1)
            fluxes = [geo[geo_at(0, a * plane, b)] * slopes[a] for a in range(points)]
            terms = contract(fluxes, deriv.T, False, skip_out=1)
            for base, value in zip(inner, terms):
                work[at(base, b)] = value
        for base in inner:
            values = [vec[at(base, b)] for b in range(points)]
            terms = in_plane(
                values,
                lambda b: geo[geo_at(1, base, b)],
                lambda b: geo[geo_at(2, base, b)],
            )
            for b in range(points):
                span = at(base, b)
                image[span] = terms[b] + work[span] + mass[span] * values[b]

    apply_inner()
    assemble_planes([(image, base) for base in inner])

    def lines_of(h):
        return range(h * points // HALVES, (h + 1) * points // HALVES)

    def meet_order(s):
        settle(near_inv.at[s], inv_send, inv_recv.at[s]).wait_recv()
        across[s] = lane_gather(near_inv[s], cell8)

    def meet(s, h):
        landed = first_in.at[s, pl.ds(0, 2 * piece)]
        settle(landed, first_send, first_recv.at[s, h]).wait_recv()
        columns = across[s]
        base = end_base(s)
        for b in lines_of(h):
            span = at(base, b)
            begin = first_out[s, line(b)] + lane_gather(first_in[s, line(b)], columns)
            whole = first_out[s, at(plane, b)] + lane_gather(first_in[s, at(plane, b)], columns)
            scaled = 1.0 / whole
            face_diag[s, line(b)] = whole
            start[span] = begin
            inverse[span] = scaled
            vec[span] = scaled * begin * (1.0 / spectrum_centre)

    def send_along(e, s, other, device):
        base = end_base(other)
        for b in range(points):
            along_out[e, s, line(b)] = (
                inner_part[e, s, line(b)] + cross[line(b)] * vec[at(base, b)]
            )
        post(
            along_out.at[e, s], along_in.at[e, 1 - s], along_send.at[e],
            along_recv.at[e, 1 - s], device,
        )

    def join_pair(s):
        columns = across[s]
        for k in (0, 1):
            for b in range(points):
                own = geo[geo_at(k + 1, s * last, b)]
                pair[s, k, line(b)] = own + lane_gather(pair_in[s, k, line(b)], columns)
        terms = contract([pair[s, 0, line(b)] for b in range(points)], square.T, True)
        for b in range(points):
            pair_diag[s, line(b)] = terms[b] + rotate_contract(pair[s, 1, line(b)], 2)

    def apply_end(s, ref):
        base = end_base(s)
        values = [vec[at(base, b)] for b in range(points)]
        terms = in_plane(values, lambda b: pair[s, 0, line(b)], lambda b: pair[s, 1, line(b)])
        for b in range(points):
            ref[at(base, b)] = terms[b] - pair_diag[s, line(b)] * values[b]

    def first_end(s):
        apply_end(s, image)
        assemble_planes([(image, end_base(s))])

    ratio_sigma = spectrum_centre / spectrum_half
    rho_prev = 1.0 / ratio_sigma
    rho_next = 1.0 / (2.0 * ratio_sigma - rho_prev)
    on_misfit = 2.0 * rho_next / spectrum_half
    on_start = (1.0 + rho_next * rho_prev) / spectrum_centre + on_misfit

    def add_ends(base, b):
        return (
            image[at(base, b)]
            + ends[0, at(base - plane, b)] * vec[at(0, b)]
            + ends[1, at(base - plane, b)] * vec[at(last, b)]
        )

    def join_along(e, s, columns, b):
        span = at(end_base(s), b)
        return (
            image[span] + face_diag[s, line(b)] * vec[span] + along_out[e, s, line(b)]
            + lane_gather(along_in[e, s, line(b)], columns)
        )

    def second_end(s):
        settle(along_in.at[0, s], along_send.at[0], along_recv.at[0, s]).wait_recv()
        columns = across[s]
        for b in range(points):
            span = at(end_base(s), b)
            total = join_along(0, s, columns, b)
            vec[span] = inverse[span] * (on_start * start[span] - on_misfit * total)

    on_load, products = [], []

    def second_inner(h):
        for b in lines_of(h):
            values = []
            for base in inner:
                span = at(base, b)
                total = add_ends(base, b)
                value = inverse[span] * (on_start * start[span] - on_misfit * total)
                vec[span] = value
                values.append(value)
            inner_to_ends(1, b, values)
            slopes = contract([None] + values + [None], deriv, False, skip_in=1)
            for a, slope in enumerate(slopes):
                products.append(geo[geo_at(0, a * plane, b)] * (slope * slope))

    def energy_inner():
        for base in inner:
            values = [vec[at(base, b)] for b in range(points)]
            slopes = contract(values, deriv, False)
            for b, value in enumerate(values):
                span = at(base, b)
                turned = rotate_contract(value, 0)
                on_load.append(load[span] * value)
                products.append(
                    geo[geo_at(1, base, b)] * (slopes[b] * slopes[b])
                    + geo[geo_at(2, base, b)] * (turned * turned)
                    + mass[span] * (value * value)
                )

    def energy_end(s):
        base = end_base(s)
        values = [vec[at(base, b)] for b in range(points)]
        slopes = contract(values, deriv, False)
        for b, value in enumerate(values):
            turned = rotate_contract(value, 0)
            weighted = share(b) * value
            on_load.append(0.5 * weighted * start[at(base, b)])
            products.append(
                0.5 * (
                    pair[s, 0, line(b)] * (slopes[b] * slopes[b])
                    + pair[s, 1, line(b)] * (turned * turned)
                    - pair_diag[s, line(b)] * (value * value)
                )
                + weighted * (0.5 * face_diag[s, line(b)] * value + 2.0 * inner_part[1, s, line(b)])
            )

    meet_order(near)
    for h in range(HALVES):
        meet(near, h)
    send_along(0, far, near, far_device)

    @pl.when(jnp.logical_not(long_way))
    def _():
        send_pair(far, far_device)

    settle(pair_in.at[near], pair_send, pair_recv.at[near]).wait_recv()
    join_pair(near)
    first_end(near)
    meet_order(far)
    for h in range(HALVES):
        meet(far, h)
        if h == HALVES - 1:
            send_along(0, near, far, near_device)
        second_inner(h)
    energy_inner()
    settle(pair_in.at[far], pair_send, pair_recv.at[far]).wait_recv()
    pl.semaphore_wait(ready, sum(w - 1 for _, w in blocks))
    join_pair(far)
    first_end(far)
    early = jnp.where(long_way, near, far)
    late = 1 - early
    early_device = jnp.where(long_way, near_device, far_device)
    late_device = jnp.where(long_way, far_device, near_device)
    second_end(early)
    send_along(1, late, early, late_device)
    energy_end(early)
    second_end(late)
    energy_end(late)
    for b in range(points):
        products.append(
            2.0 * share(b) * cross[line(b)] * vec[at(0, b)] * vec[at(last, b)]
        )
    total = jnp.concatenate(
        [jnp.sum(sum_of(part), axis=0, keepdims=True) for part in (on_load, products)], axis=1
    )

    def sum_copy(i, k):
        stride, width = strides[i], factors[i]
        return pltpu.make_async_remote_copy(
            src_ref=sums.at[i], dst_ref=parts_in[i].at[k - 1],
            send_sem=sum_send.at[i], recv_sem=sum_recv.at[i],
            device_id=(peer(stride, width, k),), device_id_type=MESH,
        )

    def start_sum(i, value):
        sums[i] = value

        @pl.loop(1, factors[i])
        def _(k):
            sum_copy(i, k).start()

    def finish_sum(i, value):
        settle(parts_in[i], sum_send.at[i], sum_recv.at[i]).wait()
        for k in range(factors[i] - 1):
            value = value + parts_in[i][k]
        return value

    start_sum(0, total)
    send_along(1, early, late, early_device)

    apply_inner()
    for s in (near, far):
        apply_end(s, image)
    assemble_planes([(image, base) for base in [0] + inner + [last]])
    for base in inner:
        for b in range(points):
            image[at(base, b)] = add_ends(base, b)
    for s in (near, far):
        settle(along_in.at[1, s], along_send.at[1], along_recv.at[1, s]).wait_recv()
        columns = across[s]
        for b in range(points):
            image[at(end_base(s), b)] = join_along(1, s, columns, b)
    settle(first_out, first_send, first_recv.at[0, 0]).wait_send()
    settle(near_inv, inv_send, inv_recv.at[0]).wait_send()
    settle(pair_in, pair_send, pair_recv.at[0]).wait_send()
    for e in (0, 1):
        settle(along_out.at[e], along_send.at[e], along_recv.at[0, 0]).wait_send()
    for i in range(len(factors)):
        if i:
            start_sum(i, total)
        total = finish_sum(i, total)
    numerator = jnp.sum(total[:, :cols], axis=1, keepdims=True)
    denominator = jnp.sum(total[:, cols:], axis=1, keepdims=True)
    size_ref[...] = jnp.broadcast_to(numerator / denominator, (points, cols))


def finish(pieces, points, start, vec, image, size, sol_hbm, res_hbm, sol, res, sems):
    rows, cols = start.shape
    scale = size[...]
    step = rows // pieces
    copies = []
    for i in range(pieces):
        part = pl.ds(i * step, step)
        for j in range(step // points):
            span = pl.ds(i * step + j * points, points)
            sol[span] = scale * vec[span]
            res[span] = start[span] - scale * image[span]
        for k, (src, dst) in enumerate(((sol, sol_hbm), (res, res_hbm))):
            copy = pltpu.make_async_copy(src.at[part], dst.at[part], sems.at[k, i])
            copy.start()
            copies.append(copy)
    for copy in copies:
        copy.wait()


PIECES = 2


def on_device(count, load_terms, geometry, mass_terms, element_order):
    points = load_terms.shape[0]
    cols = load_terms.shape[3]
    plane = points * points
    rows = points * plane
    deriv = gll_derivative(points)
    factors = radices(count)
    f32 = jnp.float32

    def room(*shape, dtype=f32):
        return pltpu.VMEM(shape + (cols,), dtype)

    dma = pltpu.SemaphoreType.DMA
    scratch = (
        [room(rows), room(3 * rows), room(rows), room(rows), room(rows)]
        + [
            room(2, 2 * plane), room(2, 2 * plane), room(2, 2, plane), room(2, 2, plane),
            room(2, plane), room(2, plane),
            room(2, rows - 2 * plane), room(plane), room(2, 2, plane),
            room(2, 2, plane), room(2, 2, plane),
            room(points, dtype=jnp.int32), room(2, points, dtype=jnp.int32),
            room(2, points, dtype=jnp.int32), room(1, dtype=jnp.int32),
            room(3, points, points),
            pltpu.VMEM((len(factors), 1, 2 * cols), f32),
        ]
        + [pltpu.VMEM((w - 1, 1, 2 * cols), f32) for w in factors]
        + [
            dma((4,)), dma, dma((2, HALVES)), dma, dma((2,)), dma, dma((2,)),
            dma((2,)), dma((2, 2)), dma((len(factors),)), dma((len(factors),)),
            pltpu.SemaphoreType.REGULAR,
        ]
    )
    hbm = pl.BlockSpec(memory_space=pl.ANY)
    vmem = pl.BlockSpec(memory_space=pltpu.VMEM)
    pieces = pl.pallas_call(
        functools.partial(kernel, count, points, factors, deriv),
        out_shape=(pltpu.VMEM((rows, cols), f32),) * 3 + (pltpu.VMEM((points, cols), f32),),
        in_specs=[hbm] * 4,
        out_specs=(vmem,) * 4,
        scratch_shapes=scratch,
        compiler_params=pltpu.CompilerParams(collective_id=0, has_side_effects=True),
    )(
        load_terms.reshape(rows, cols),
        geometry.reshape(3 * rows, cols),
        mass_terms.reshape(rows, cols),
        element_order,
    )
    solution_rows, residual_rows = pl.pallas_call(
        functools.partial(finish, PIECES, points),
        out_shape=(jax.ShapeDtypeStruct((rows, cols), f32),) * 2,
        in_specs=[vmem] * 4,
        out_specs=(hbm, hbm),
        scratch_shapes=[room(rows), room(rows), dma((2, PIECES))],
        compiler_params=pltpu.CompilerParams(vmem_limit_bytes=8 * rows * cols * 4),
    )(*pieces)
    shape = load_terms.shape
    return solution_rows.reshape(shape), residual_rows.reshape(shape)


def solution(mesh):
    placed = (
        P(None, None, None, "slab"),
        P(None, None, None, None, "slab"),
        P(None, None, None, "slab"),
        P("slab", None),
    )
    return jax.shard_map(
        functools.partial(on_device, mesh.shape["slab"]),
        mesh=mesh,
        in_specs=placed,
        out_specs=(P(None, None, None, "slab"), P(None, None, None, "slab")),
        check_vma=False,
    )
```

```python
import functools

import jax
import jax.numpy as jnp
import numpy as np
from jax import lax
from jax.experimental import pallas as pl
from jax.experimental.pallas import tpu as pltpu
from jax.sharding import PartitionSpec as P

EL_Y = 8
EL_Z = 16
MESH = pl.DeviceIdType.MESH
WIDEST = 32
HALVES = 2

spectrum_centre = 1.65
spectrum_half = 1.35


def legendre_table(positions, points):
    columns = [positions * 0.0 + 1.0, positions]
    for degree_now in range(2, points):
        columns.append(
            ((2 * degree_now - 1) * positions * columns[-1] - (degree_now - 1) * columns[-2])
            / degree_now
        )
    return np.stack(columns, axis=1)


def gll_derivative(points):
    degree = points - 1
    grid_nodes = -np.cos(np.pi * np.arange(points) / degree)
    for repeat in range(100):
        legendre = legendre_table(grid_nodes, points)
        grid_nodes = grid_nodes - (grid_nodes * legendre[:, degree] - legendre[:, degree - 1]) / (
            points * legendre[:, degree]
        )
    legendre = legendre_table(grid_nodes, points)
    top_values = legendre[:, degree]
    index_list = np.arange(points)
    same_index = index_list[:, None] == index_list[None, :]
    spacing = grid_nodes[:, None] - grid_nodes[None, :]
    spacing = np.where(same_index, 1.0, spacing)
    deriv_table = top_values[:, None] / (top_values[None, :] * spacing)
    deriv_table = np.where(same_index, 0.0, deriv_table)
    deriv_table[0, 0] = -degree * points / 4.0
    deriv_table[degree, degree] = degree * points / 4.0
    return deriv_table


def radices(count):
    factors = []
    while count > 1:
        width = max([w for w in range(2, WIDEST + 1) if count % w == 0], default=count)
        factors.append(width)
        count //= width
    return factors


def square_split(width):
    return min(d for d in range(1, width + 1) if width % d == 0 and d * d >= width)


def contract(values, table, symmetric, skip_in=0, skip_out=0):
    points = len(values)
    half = points // 2
    ins = range(skip_in, half)
    even = {j: values[j] + values[points - 1 - j] for j in ins}
    odd = {j: values[j] - values[points - 1 - j] for j in ins}
    low, high = [], []
    for m in range(skip_out, half):
        part_even, part_odd = None, None
        for j in ins:
            a = float(0.5 * (table[m, j] + table[m, points - 1 - j]))
            b = float(0.5 * (table[m, j] - table[m, points - 1 - j]))
            part_even = a * even[j] if part_even is None else part_even + a * even[j]
            part_odd = b * odd[j] if part_odd is None else part_odd + b * odd[j]
        low.append(part_even + part_odd)
        high.append(part_even - part_odd if symmetric else part_odd - part_even)
    return low + high[::-1]


def end_columns(values, deriv):
    points = len(values)
    half = points // 2
    even = [values[m] + values[points - 1 - m] for m in range(half)]
    odd = [values[m] - values[points - 1 - m] for m in range(half)]
    low, high = {}, {}
    for a in range(1, points - 1):
        product = deriv[:, 0] * deriv[:, a]
        part_even, part_odd = None, None
        for m in range(half):
            p = float(0.5 * (product[m] + product[points - 1 - m]))
            q = float(0.5 * (product[m] - product[points - 1 - m]))
            part_even = p * even[m] if part_even is None else part_even + p * even[m]
            part_odd = q * odd[m] if part_odd is None else part_odd + q * odd[m]
        low[a] = part_even + part_odd
        high[points - 1 - a] = part_even - part_odd
    product = deriv[:, 0] * deriv[:, points - 1]
    cross = float(product[0]) * even[0]
    for m in range(1, half):
        cross = cross + float(product[m]) * even[m]
    return low, high, cross


def sum_of(terms):
    while len(terms) > 1:
        terms = [x + y for x, y in zip(terms[::2], terms[1::2])] + terms[len(terms) & ~1:]
    return terms[0]


def lane_gather(values, columns):
    dims = lax.GatherDimensionNumbers(
        offset_dims=(),
        collapsed_slice_dims=(1,),
        start_index_map=(1,),
        operand_batching_dims=(0,),
        start_indices_batching_dims=(0,),
    )
    return lax.gather(
        values, columns[..., None], dims, (1, 1), mode=lax.GatherScatterMode.PROMISE_IN_BOUNDS
    )


def kernel(
    count, points, factors, deriv,
    load_hbm, geo_hbm, mass_hbm, order_hbm, start, vec, image, size_ref,
    load, geo, mass, inverse, work,
    first_out, first_in, pair_in, pair, pair_diag, face_diag,
    ends, cross, inner_part, along_out, along_in,
    relay_inv, relay_first, relay_pair, relay_along,
    own_inv, near_inv, across, order, coef, sums, *rest,
):
    parts_in = rest[: len(factors)]
    (
        in_sem, first_send, first_recv, inv_send, inv_recv, pair_send, pair_recv,
        along_send, along_recv, sum_send, sum_recv, ready, mate_ready, relay_send, relay_recv,
    ) = rest[len(factors):]
    me = lax.axis_index("slab")
    right = lax.rem(me + 1, count)
    left = lax.rem(me + count - 1, count)
    plane = points * points
    rows = points * plane
    last = rows - plane
    piece = plane // HALVES
    cols = load.shape[1]
    odd_one = lax.rem(me, 2)
    near = 1 - odd_one
    far = odd_one
    near_device = lax.rem(me + count + 1 - 2 * odd_one, count)
    far_device = lax.rem(me + count - 1 + 2 * odd_one, count)
    long_way = lax.rem((me + 1) // 2, 2) == 0

    fetch = [
        pltpu.make_async_copy(geo_hbm, geo, in_sem.at[0]),
        pltpu.make_async_copy(mass_hbm, mass, in_sem.at[1]),
        pltpu.make_async_copy(load_hbm, load, in_sem.at[2]),
        pltpu.make_async_copy(order_hbm, order, in_sem.at[3]),
    ]

    def peer(stride, width, k):
        digit = lax.rem(me // stride, width)
        return me + (lax.rem(digit + k, width) - digit) * stride

    strides = [int(np.prod(factors[:i])) for i in range(len(factors))]
    blocks = [(stride, square_split(width)) for stride, width in zip(strides, factors)]
    columns_of = [
        (stride * size, width // size) for (stride, size), width in zip(blocks, factors)
    ]

    groups = blocks + columns_of
    relay = blocks[0][1] + 1
    first_chip = me <= 1
    barrier = pltpu.get_barrier_semaphore()

    def signal(semaphore, device):
        pl.semaphore_signal(semaphore, inc=1, device_id=(device,), device_id_type=MESH)

    def greet(semaphore, among, wanted, beside=()):
        for device in beside:
            @pl.when(wanted(device))
            def _():
                signal(semaphore, device)

        for stride, width in among:
            @pl.loop(1, width)
            def _(k):
                device = peer(stride, width, k)

                @pl.when(wanted(device))
                def _():
                    signal(semaphore, device)

    @pl.when(me == count - 1)
    def _():
        signal(barrier, relay)

    @pl.when((me == 1) | (me == relay))
    def _():
        signal(barrier, 0)

    @pl.when(me == 0)
    def _():
        signal(barrier, 1)

    for copy in fetch[::-1][:1] + fetch[:3]:
        copy.start()
    greet(barrier, groups, lambda device: device > 1, (left, right))

    fetch[3].wait()
    cell = order[...]
    cell8 = jnp.broadcast_to(cell, (points, cols))
    cell_col = jnp.transpose(jnp.broadcast_to(cell.astype(jnp.float32), (cols, cols)))
    lane = lax.broadcasted_iota(jnp.int32, (cols, cols), 1).astype(jnp.float32)
    source = lax.broadcasted_iota(jnp.int32, (cols, cols), 0).astype(jnp.float32)
    inv_row = jnp.sum(jnp.where(cell_col == lane, source, 0.0), axis=0, keepdims=True)
    inv8 = jnp.broadcast_to(inv_row.astype(jnp.int32), (points, cols))
    own_inv[...] = inv8
    pos_z = cell8 % EL_Z
    has_up = cell8 < cols - EL_Z
    has_down = cell8 >= EL_Z
    plus_y = lane_gather(inv8, jnp.where(has_up, cell8 + EL_Z, cell8))
    minus_y = lane_gather(inv8, jnp.where(has_down, cell8 - EL_Z, cell8))
    plus_z = lane_gather(inv8, jnp.where(pos_z == EL_Z - 1, cell8 - (EL_Z - 1), cell8 + 1))
    minus_z = lane_gather(inv8, jnp.where(pos_z == 0, cell8 + (EL_Z - 1), cell8 - 1))

    row_id = lax.broadcasted_iota(jnp.int32, (points, cols), 0)
    for t, table in enumerate((deriv, deriv.T, (deriv * deriv).T)):
        for k in range(points):
            vector = jnp.zeros((points, cols), jnp.float32)
            for m in range(points):
                vector = jnp.where(row_id == m, float(table[m, (m - k) % points]), vector)
            coef[t, k] = vector
    share_z = jnp.where((row_id == 0) | (row_id == points - 1), 0.5, 1.0)
    share_low = jnp.where(has_down, 0.5 * share_z, share_z)
    share_high = jnp.where(has_up, 0.5 * share_z, share_z)

    def share(b):
        return share_low if b == 0 else share_high if b == points - 1 else share_z

    def rotate_contract(value, t):
        total = coef[t, 0] * value
        for k in range(1, points):
            total = total + coef[t, k] * pltpu.roll(value, k, 0)
        return total

    def post(src, dst, send_sem, recv_sem, device):
        pltpu.make_async_remote_copy(
            src_ref=src, dst_ref=dst, send_sem=send_sem, recv_sem=recv_sem,
            device_id=(device,), device_id_type=MESH,
        ).start()

    def settle(ref, send_sem, recv_sem):
        return pltpu.make_async_remote_copy(
            src_ref=ref, dst_ref=ref, send_sem=send_sem, recv_sem=recv_sem,
            device_id=(right,), device_id_type=MESH,
        )

    def line(b):
        return pl.ds(b * points, points)

    def at(base, b):
        if isinstance(base, int):
            return pl.ds(base + b * points, points)
        return pl.ds(pl.multiple_of(base + b * points, points), points)

    def geo_at(k, base, b):
        return at(k * rows + base, b)

    def end_base(s):
        return pl.multiple_of(s * last, points)

    inner = [a * plane for a in range(1, points - 1)]

    def assemble_planes(spots):
        lows = [ref[at(base, 0)] for ref, base in spots]
        highs = [ref[at(base, points - 1)] for ref, base in spots]
        from_low = [lane_gather(low, plus_y) for low in lows]
        from_high = [lane_gather(high, minus_y) for high in highs]
        for i, (ref, base) in enumerate(spots):
            ref[at(base, points - 1)] = highs[i] + jnp.where(has_up, from_low[i], 0.0)
            ref[at(base, 0)] = lows[i] + jnp.where(has_down, from_high[i], 0.0)
        firsts = [pl.ds(base, points, stride=points) for _, base in spots]
        ends_at = [pl.ds(base + points - 1, points, stride=points) for _, base in spots]
        lows = [ref[first] for (ref, _), first in zip(spots, firsts)]
        highs = [ref[end] for (ref, _), end in zip(spots, ends_at)]
        from_low = [lane_gather(low, plus_z) for low in lows]
        from_high = [lane_gather(high, minus_z) for high in highs]
        for i, (ref, _) in enumerate(spots):
            ref[ends_at[i]] = highs[i] + from_low[i]
            ref[firsts[i]] = lows[i] + from_high[i]

    square = deriv * deriv
    fetch[0].wait()
    fetch[1].wait()

    for b in range(points):
        values = [geo[geo_at(0, a * plane, b)] for a in range(points)]
        for a, value in enumerate(contract(values, square.T, True)):
            work[at(a * plane, b)] = value

    def diagonal_plane(base, put):
        values = [geo[geo_at(1, base, b)] for b in range(points)]
        for b, value in enumerate(contract(values, square.T, True)):
            value = value + rotate_contract(geo[geo_at(2, base, b)], 2)
            put(b, value + work[at(base, b)] + mass[at(base, b)])

    for s, base in ((0, 0), (1, last)):

        def put(b, value):
            first_out[s, at(plane, b)] = value

        diagonal_plane(base, put)
    fetch[2].wait()
    for s, base in ((0, 0), (1, last)):
        for b in range(points):
            first_out[s, line(b)] = load[at(base, b)]
    assemble_planes([(first_out.at[s], k * plane) for s in (0, 1) for k in (0, 1)])

    for base in inner:
        for b in range(points):
            start[at(base, b)] = load[at(base, b)]

        def put(b, value):
            inverse[at(base, b)] = value

        diagonal_plane(base, put)
    assemble_planes([(ref, base) for base in inner for ref in (start, inverse)])
    for base in inner:
        for b in range(points):
            span = at(base, b)
            scaled = 1.0 / inverse[span]
            inverse[span] = scaled
            vec[span] = scaled * start[span] * (1.0 / spectrum_centre)
    for b in range(points):
        values = [geo[geo_at(0, a * plane, b)] for a in range(points)]
        low, high, both = end_columns(values, deriv)
        for a in range(1, points - 1):
            ends[0, at((a - 1) * plane, b)] = low[a]
            ends[1, at((a - 1) * plane, b)] = high[a]
        cross[line(b)] = both
    assemble_planes(
        [(ends.at[s], base - plane) for s in (0, 1) for base in inner] + [(cross, 0)]
    )

    def inner_to_ends(e, b, values):
        for s in (0, 1):
            inner_part[e, s, line(b)] = sum_of(
                [ends[s, at(base - plane, b)] * v for base, v in zip(inner, values)]
            )

    for b in range(points):
        inner_to_ends(0, b, [vec[at(base, b)] for base in inner])

    in_block = sum(w - 1 for _, w in blocks)
    in_groups = sum(w - 1 for _, w in groups)
    callers = jnp.where(me == 0, 2, jnp.where(me == 1, 1, 2 + in_groups))
    pl.semaphore_wait(barrier, callers + jnp.where(me == relay, 1, 0))

    def halves_of():
        return [
            (h, pl.ds(k * plane + h * piece, piece)) for h in range(HALVES) for k in (0, 1)
        ]

    def send_first(s, device):
        post(own_inv, near_inv.at[1 - s], inv_send, inv_recv.at[1 - s], device)
        for h, part in halves_of():
            post(
                first_out.at[s, part], first_in.at[1 - s, part], first_send,
                first_recv.at[1 - s, h], device,
            )

    def pair_source(s, k):
        return geo.at[pl.ds(pl.multiple_of((k + 1) * rows + s * last, points), plane)]

    def send_pair(s, device):
        for k in (0, 1):
            post(
                pair_source(s, k), pair_in.at[1 - s, k], pair_send, pair_recv.at[1 - s], device
            )

    @pl.when(me == 0)
    def _():
        post(own_inv, relay_inv, inv_send, relay_recv.at[HALVES + 2], relay)
        for h, part in halves_of():
            post(first_out.at[0, part], relay_first.at[part], first_send, relay_recv.at[h], relay)
        for k in (0, 1):
            post(pair_source(0, k), relay_pair.at[k], pair_send, relay_recv.at[HALVES], relay)

    @pl.when(jnp.logical_not(first_chip))
    def _():
        send_first(far, far_device)
        send_pair(far, far_device)

    send_first(near, near_device)
    send_pair(near, near_device)

    @pl.when(jnp.logical_not(first_chip))
    def _():
        greet(ready, blocks, lambda device: device >= 0)
        greet(ready, columns_of, lambda device: device <= 1, (left, right))

    @pl.when(me == relay)
    def _():
        end = count - 1
        settle(relay_inv, relay_send, relay_recv.at[HALVES + 2]).wait_recv()
        post(relay_inv, near_inv.at[1], relay_send, inv_recv.at[1], end)
        for h in range(HALVES):
            landed = relay_first.at[pl.ds(0, 2 * piece)]
            settle(landed, relay_send, relay_recv.at[h]).wait_recv()
            for at_half, part in halves_of():
                if at_half == h:
                    post(
                        relay_first.at[part], first_in.at[1, part], relay_send,
                        first_recv.at[1, h], end,
                    )
        settle(relay_pair, relay_send, relay_recv.at[HALVES]).wait_recv()
        for k in (0, 1):
            post(relay_pair.at[k], pair_in.at[1, k], relay_send, pair_recv.at[1], end)

    def in_plane(values, slope_geo, flux_geo):
        slopes = contract(values, deriv, False)
        fluxes = [slope_geo(b) * slopes[b] for b in range(points)]
        out = contract(fluxes, deriv.T, False)
        for b in range(points):
            flux = flux_geo(b) * rotate_contract(values[b], 0)
            out[b] = out[b] + rotate_contract(flux, 1)
        return out

    def apply_inner():
        for b in range(points):
            values = [None] + [vec[at(base, b)] for base in inner] + [None]
            slopes = contract(values, deriv, False, skip_in=1)
            fluxes = [geo[geo_at(0, a * plane, b)] * slopes[a] for a in range(points)]
            terms = contract(fluxes, deriv.T, False, skip_out=1)
            for base, value in zip(inner, terms):
                work[at(base, b)] = value
        for base in inner:
            values = [vec[at(base, b)] for b in range(points)]
            terms = in_plane(
                values,
                lambda b: geo[geo_at(1, base, b)],
                lambda b: geo[geo_at(2, base, b)],
            )
            for b in range(points):
                span = at(base, b)
                image[span] = terms[b] + work[span] + mass[span] * values[b]

    apply_inner()
    assemble_planes([(image, base) for base in inner])

    def lines_of(h):
        return range(h * points // HALVES, (h + 1) * points // HALVES)

    def meet_order(s):
        settle(near_inv.at[s], inv_send, inv_recv.at[s]).wait_recv()
        across[s] = lane_gather(near_inv[s], cell8)

    def meet(s, h):
        landed = first_in.at[s, pl.ds(0, 2 * piece)]
        settle(landed, first_send, first_recv.at[s, h]).wait_recv()
        columns = across[s]
        base = end_base(s)
        for b in lines_of(h):
            span = at(base, b)
            begin = first_out[s, line(b)] + lane_gather(first_in[s, line(b)], columns)
            whole = first_out[s, at(plane, b)] + lane_gather(first_in[s, at(plane, b)], columns)
            scaled = 1.0 / whole
            face_diag[s, line(b)] = whole
            start[span] = begin
            inverse[span] = scaled
            vec[span] = scaled * begin * (1.0 / spectrum_centre)

    def put_along(e, s, other):
        base = end_base(other)
        for b in range(points):
            along_out[e, s, line(b)] = (
                inner_part[e, s, line(b)] + cross[line(b)] * vec[at(base, b)]
            )

    def post_along(e, s, device):
        post(
            along_out.at[e, s], along_in.at[e, 1 - s], along_send.at[e],
            along_recv.at[e, 1 - s], device,
        )

    def send_along(e, s, other, device):
        put_along(e, s, other)
        post_along(e, s, device)

    def join_pair(s):
        columns = across[s]
        for k in (0, 1):
            for b in range(points):
                own = geo[geo_at(k + 1, s * last, b)]
                pair[s, k, line(b)] = own + lane_gather(pair_in[s, k, line(b)], columns)
        terms = contract([pair[s, 0, line(b)] for b in range(points)], square.T, True)
        for b in range(points):
            pair_diag[s, line(b)] = terms[b] + rotate_contract(pair[s, 1, line(b)], 2)

    def apply_end(s, ref):
        base = end_base(s)
        values = [vec[at(base, b)] for b in range(points)]
        terms = in_plane(values, lambda b: pair[s, 0, line(b)], lambda b: pair[s, 1, line(b)])
        for b in range(points):
            ref[at(base, b)] = terms[b] - pair_diag[s, line(b)] * values[b]

    def first_end(s):
        apply_end(s, image)
        assemble_planes([(image, end_base(s))])

    ratio_sigma = spectrum_centre / spectrum_half
    rho_prev = 1.0 / ratio_sigma
    rho_next = 1.0 / (2.0 * ratio_sigma - rho_prev)
    on_misfit = 2.0 * rho_next / spectrum_half
    on_start = (1.0 + rho_next * rho_prev) / spectrum_centre + on_misfit

    def add_ends(base, b):
        return (
            image[at(base, b)]
            + ends[0, at(base - plane, b)] * vec[at(0, b)]
            + ends[1, at(base - plane, b)] * vec[at(last, b)]
        )

    def join_along(e, s, columns, b):
        span = at(end_base(s), b)
        return (
            image[span] + face_diag[s, line(b)] * vec[span] + along_out[e, s, line(b)]
            + lane_gather(along_in[e, s, line(b)], columns)
        )

    def second_end(s):
        settle(along_in.at[0, s], along_send.at[0], along_recv.at[0, s]).wait_recv()
        columns = across[s]
        for b in range(points):
            span = at(end_base(s), b)
            total = join_along(0, s, columns, b)
            vec[span] = inverse[span] * (on_start * start[span] - on_misfit * total)

    on_load, products = [], []

    def second_inner(h):
        for b in lines_of(h):
            values = []
            for base in inner:
                span = at(base, b)
                total = add_ends(base, b)
                value = inverse[span] * (on_start * start[span] - on_misfit * total)
                vec[span] = value
                values.append(value)
            inner_to_ends(1, b, values)
            slopes = contract([None] + values + [None], deriv, False, skip_in=1)
            for a, slope in enumerate(slopes):
                products.append(geo[geo_at(0, a * plane, b)] * (slope * slope))

    def energy_inner():
        for base in inner:
            values = [vec[at(base, b)] for b in range(points)]
            slopes = contract(values, deriv, False)
            for b, value in enumerate(values):
                span = at(base, b)
                turned = rotate_contract(value, 0)
                on_load.append(load[span] * value)
                products.append(
                    geo[geo_at(1, base, b)] * (slopes[b] * slopes[b])
                    + geo[geo_at(2, base, b)] * (turned * turned)
                    + mass[span] * (value * value)
                )

    def energy_end(s):
        base = end_base(s)
        values = [vec[at(base, b)] for b in range(points)]
        slopes = contract(values, deriv, False)
        for b, value in enumerate(values):
            turned = rotate_contract(value, 0)
            weighted = share(b) * value
            on_load.append(0.5 * weighted * start[at(base, b)])
            products.append(
                0.5 * (
                    pair[s, 0, line(b)] * (slopes[b] * slopes[b])
                    + pair[s, 1, line(b)] * (turned * turned)
                    - pair_diag[s, line(b)] * (value * value)
                )
                + weighted * (0.5 * face_diag[s, line(b)] * value + 2.0 * inner_part[1, s, line(b)])
            )

    meet_order(near)
    for h in range(HALVES):
        meet(near, h)
    put_along(0, far, near)

    @pl.when(jnp.logical_not(first_chip))
    def _():
        post_along(0, far, far_device)

    @pl.when(me == 0)
    def _():
        post(
            along_out.at[0, 0], relay_along, along_send.at[0], relay_recv.at[HALVES + 1], relay
        )

    @pl.when(me == relay)
    def _():
        settle(relay_along, relay_send, relay_recv.at[HALVES + 1]).wait_recv()
        post(relay_along, along_in.at[0, 1], relay_send, along_recv.at[0, 1], count - 1)

    @pl.when(first_chip)
    def _():
        pl.semaphore_wait(ready, in_groups)
        greet(ready, blocks, lambda device: device > 1)
        signal(mate_ready, 1 - me)

        @pl.when(me == 1)
        def _():
            send_first(far, far_device)
            post_along(0, far, far_device)
            send_pair(far, far_device)

    settle(pair_in.at[near], pair_send, pair_recv.at[near]).wait_recv()
    join_pair(near)
    first_end(near)
    meet_order(far)
    for h in range(HALVES):
        meet(far, h)
        if h == HALVES - 1:
            send_along(0, near, far, near_device)
        second_inner(h)
    energy_inner()
    settle(pair_in.at[far], pair_send, pair_recv.at[far]).wait_recv()

    @pl.when(first_chip)
    def _():
        pl.semaphore_wait(mate_ready, 1)

    @pl.when(jnp.logical_not(first_chip))
    def _():
        pl.semaphore_wait(ready, in_block)

    join_pair(far)
    first_end(far)
    early = jnp.where(long_way, near, far)
    late = 1 - early
    early_device = jnp.where(long_way, near_device, far_device)
    late_device = jnp.where(long_way, far_device, near_device)
    second_end(early)
    send_along(1, late, early, late_device)
    energy_end(early)
    second_end(late)
    energy_end(late)
    for b in range(points):
        products.append(
            2.0 * share(b) * cross[line(b)] * vec[at(0, b)] * vec[at(last, b)]
        )
    total = jnp.concatenate(
        [jnp.sum(sum_of(part), axis=0, keepdims=True) for part in (on_load, products)], axis=1
    )

    def sum_copy(i, k):
        stride, width = strides[i], factors[i]
        return pltpu.make_async_remote_copy(
            src_ref=sums.at[i], dst_ref=parts_in[i].at[k - 1],
            send_sem=sum_send.at[i], recv_sem=sum_recv.at[i],
            device_id=(peer(stride, width, k),), device_id_type=MESH,
        )

    def start_sum(i, value):
        sums[i] = value

        @pl.loop(1, factors[i])
        def _(k):
            sum_copy(i, k).start()

    def finish_sum(i, value):
        settle(parts_in[i], sum_send.at[i], sum_recv.at[i]).wait()
        for k in range(factors[i] - 1):
            value = value + parts_in[i][k]
        return value

    start_sum(0, total)
    send_along(1, early, late, early_device)

    apply_inner()
    for s in (near, far):
        apply_end(s, image)
    assemble_planes([(image, base) for base in [0] + inner + [last]])
    for base in inner:
        for b in range(points):
            image[at(base, b)] = add_ends(base, b)
    for s in (near, far):
        settle(along_in.at[1, s], along_send.at[1], along_recv.at[1, s]).wait_recv()
        columns = across[s]
        for b in range(points):
            image[at(end_base(s), b)] = join_along(1, s, columns, b)
    settle(first_out, first_send, first_recv.at[0, 0]).wait_send()
    settle(near_inv, inv_send, inv_recv.at[0]).wait_send()
    settle(pair_in, pair_send, pair_recv.at[0]).wait_send()
    for e in (0, 1):
        settle(along_out.at[e], along_send.at[e], along_recv.at[0, 0]).wait_send()

    @pl.when(me == relay)
    def _():
        for ref in (relay_inv, relay_first, relay_pair, relay_along):
            settle(ref, relay_send, relay_recv.at[0]).wait_send()

    for i in range(len(factors)):
        if i:
            start_sum(i, total)
        total = finish_sum(i, total)
    numerator = jnp.sum(total[:, :cols], axis=1, keepdims=True)
    denominator = jnp.sum(total[:, cols:], axis=1, keepdims=True)
    size_ref[...] = jnp.broadcast_to(numerator / denominator, (points, cols))


def finish(pieces, points, start, vec, image, size, sol_hbm, res_hbm, sol, res, sems):
    rows, cols = start.shape
    scale = size[...]
    step = rows // pieces
    copies = []
    for i in range(pieces):
        part = pl.ds(i * step, step)
        for j in range(step // points):
            span = pl.ds(i * step + j * points, points)
            sol[span] = scale * vec[span]
            res[span] = start[span] - scale * image[span]
        for k, (src, dst) in enumerate(((sol, sol_hbm), (res, res_hbm))):
            copy = pltpu.make_async_copy(src.at[part], dst.at[part], sems.at[k, i])
            copy.start()
            copies.append(copy)
    for copy in copies:
        copy.wait()


PIECES = 2


def on_device(count, load_terms, geometry, mass_terms, element_order):
    points = load_terms.shape[0]
    cols = load_terms.shape[3]
    plane = points * points
    rows = points * plane
    deriv = gll_derivative(points)
    factors = radices(count)
    f32 = jnp.float32

    def room(*shape, dtype=f32):
        return pltpu.VMEM(shape + (cols,), dtype)

    dma = pltpu.SemaphoreType.DMA
    scratch = (
        [room(rows), room(3 * rows), room(rows), room(rows), room(rows)]
        + [
            room(2, 2 * plane), room(2, 2 * plane), room(2, 2, plane), room(2, 2, plane),
            room(2, plane), room(2, plane),
            room(2, rows - 2 * plane), room(plane), room(2, 2, plane),
            room(2, 2, plane), room(2, 2, plane),
            room(points, dtype=jnp.int32), room(2 * plane), room(2, plane), room(plane),
            room(points, dtype=jnp.int32), room(2, points, dtype=jnp.int32),
            room(2, points, dtype=jnp.int32), room(1, dtype=jnp.int32),
            room(3, points, points),
            pltpu.VMEM((len(factors), 1, 2 * cols), f32),
        ]
        + [pltpu.VMEM((w - 1, 1, 2 * cols), f32) for w in factors]
        + [
            dma((4,)), dma, dma((2, HALVES)), dma, dma((2,)), dma, dma((2,)),
            dma((2,)), dma((2, 2)), dma((len(factors),)), dma((len(factors),)),
            pltpu.SemaphoreType.REGULAR, pltpu.SemaphoreType.REGULAR,
            dma, dma((HALVES + 3,)),
        ]
    )
    hbm = pl.BlockSpec(memory_space=pl.ANY)
    vmem = pl.BlockSpec(memory_space=pltpu.VMEM)
    pieces = pl.pallas_call(
        functools.partial(kernel, count, points, factors, deriv),
        out_shape=(pltpu.VMEM((rows, cols), f32),) * 3 + (pltpu.VMEM((points, cols), f32),),
        in_specs=[hbm] * 4,
        out_specs=(vmem,) * 4,
        scratch_shapes=scratch,
        compiler_params=pltpu.CompilerParams(collective_id=0, has_side_effects=True),
    )(
        load_terms.reshape(rows, cols),
        geometry.reshape(3 * rows, cols),
        mass_terms.reshape(rows, cols),
        element_order,
    )
    solution_rows, residual_rows = pl.pallas_call(
        functools.partial(finish, PIECES, points),
        out_shape=(jax.ShapeDtypeStruct((rows, cols), f32),) * 2,
        in_specs=[vmem] * 4,
        out_specs=(hbm, hbm),
        scratch_shapes=[room(rows), room(rows), dma((2, PIECES))],
        compiler_params=pltpu.CompilerParams(vmem_limit_bytes=8 * rows * cols * 4),
    )(*pieces)
    shape = load_terms.shape
    return solution_rows.reshape(shape), residual_rows.reshape(shape)


def solution(mesh):
    placed = (
        P(None, None, None, "slab"),
        P(None, None, None, None, "slab"),
        P(None, None, None, "slab"),
        P("slab", None),
    )
    return jax.shard_map(
        functools.partial(on_device, mesh.shape["slab"]),
        mesh=mesh,
        in_specs=placed,
        out_specs=(P(None, None, None, "slab"), P(None, None, None, "slab")),
        check_vma=False,
    )
```

```python
import functools

import jax
import jax.numpy as jnp
import numpy as np
from jax import lax
from jax.experimental import pallas as pl
from jax.experimental.pallas import tpu as pltpu
from jax.sharding import PartitionSpec as P

EL_Y = 8
EL_Z = 16
MESH = pl.DeviceIdType.MESH
WIDEST = 32
HALVES = 2

spectrum_centre = 1.65
spectrum_half = 1.35


def legendre_table(positions, points):
    columns = [positions * 0.0 + 1.0, positions]
    for degree_now in range(2, points):
        columns.append(
            ((2 * degree_now - 1) * positions * columns[-1] - (degree_now - 1) * columns[-2])
            / degree_now
        )
    return np.stack(columns, axis=1)


def gll_derivative(points):
    degree = points - 1
    grid_nodes = -np.cos(np.pi * np.arange(points) / degree)
    for repeat in range(100):
        legendre = legendre_table(grid_nodes, points)
        grid_nodes = grid_nodes - (grid_nodes * legendre[:, degree] - legendre[:, degree - 1]) / (
            points * legendre[:, degree]
        )
    legendre = legendre_table(grid_nodes, points)
    top_values = legendre[:, degree]
    index_list = np.arange(points)
    same_index = index_list[:, None] == index_list[None, :]
    spacing = grid_nodes[:, None] - grid_nodes[None, :]
    spacing = np.where(same_index, 1.0, spacing)
    deriv_table = top_values[:, None] / (top_values[None, :] * spacing)
    deriv_table = np.where(same_index, 0.0, deriv_table)
    deriv_table[0, 0] = -degree * points / 4.0
    deriv_table[degree, degree] = degree * points / 4.0
    return deriv_table


def radices(count):
    factors = []
    while count > 1:
        width = max([w for w in range(2, WIDEST + 1) if count % w == 0], default=count)
        factors.append(width)
        count //= width
    return factors


def square_split(width):
    return min(d for d in range(1, width + 1) if width % d == 0 and d * d >= width)


def contract(values, table, symmetric, skip_in=0, skip_out=0):
    points = len(values)
    half = points // 2
    ins = range(skip_in, half)
    even = {j: values[j] + values[points - 1 - j] for j in ins}
    odd = {j: values[j] - values[points - 1 - j] for j in ins}
    low, high = [], []
    for m in range(skip_out, half):
        part_even, part_odd = None, None
        for j in ins:
            a = float(0.5 * (table[m, j] + table[m, points - 1 - j]))
            b = float(0.5 * (table[m, j] - table[m, points - 1 - j]))
            part_even = a * even[j] if part_even is None else part_even + a * even[j]
            part_odd = b * odd[j] if part_odd is None else part_odd + b * odd[j]
        low.append(part_even + part_odd)
        high.append(part_even - part_odd if symmetric else part_odd - part_even)
    return low + high[::-1]


def end_columns(values, deriv):
    points = len(values)
    half = points // 2
    even = [values[m] + values[points - 1 - m] for m in range(half)]
    odd = [values[m] - values[points - 1 - m] for m in range(half)]
    low, high = {}, {}
    for a in range(1, points - 1):
        product = deriv[:, 0] * deriv[:, a]
        part_even, part_odd = None, None
        for m in range(half):
            p = float(0.5 * (product[m] + product[points - 1 - m]))
            q = float(0.5 * (product[m] - product[points - 1 - m]))
            part_even = p * even[m] if part_even is None else part_even + p * even[m]
            part_odd = q * odd[m] if part_odd is None else part_odd + q * odd[m]
        low[a] = part_even + part_odd
        high[points - 1 - a] = part_even - part_odd
    product = deriv[:, 0] * deriv[:, points - 1]
    cross = float(product[0]) * even[0]
    for m in range(1, half):
        cross = cross + float(product[m]) * even[m]
    return low, high, cross


def sum_of(terms):
    while len(terms) > 1:
        terms = [x + y for x, y in zip(terms[::2], terms[1::2])] + terms[len(terms) & ~1:]
    return terms[0]


def lane_gather(values, columns):
    dims = lax.GatherDimensionNumbers(
        offset_dims=(),
        collapsed_slice_dims=(1,),
        start_index_map=(1,),
        operand_batching_dims=(0,),
        start_indices_batching_dims=(0,),
    )
    return lax.gather(
        values, columns[..., None], dims, (1, 1), mode=lax.GatherScatterMode.PROMISE_IN_BOUNDS
    )


def kernel(
    count, points, factors, deriv,
    load_hbm, geo_hbm, mass_hbm, order_hbm, start, vec, image, size_ref,
    load, geo, mass, inverse, work,
    first_out, first_in, pair_in, pair, pair_diag, face_diag,
    ends, cross, inner_part, along_out, along_in,
    relay_inv, relay_first, relay_pair, relay_along,
    own_inv, near_inv, across, order, coef, sums, *rest,
):
    parts_in = rest[: len(factors)]
    (
        in_sem, sends, first_recv, pair_recv, along_recv, sum_send, sum_recv, ready, mate_ready,
        relay_recv,
    ) = rest[len(factors):]
    me = lax.axis_index("slab")
    right = lax.rem(me + 1, count)
    left = lax.rem(me + count - 1, count)
    plane = points * points
    rows = points * plane
    last = rows - plane
    piece = plane // HALVES
    cols = load.shape[1]
    odd_one = lax.rem(me, 2)
    near = 1 - odd_one
    far = odd_one
    near_device = lax.rem(me + count + 1 - 2 * odd_one, count)
    far_device = lax.rem(me + count - 1 + 2 * odd_one, count)
    long_way = lax.rem((me + 1) // 2, 2) == 0

    fetch = [
        pltpu.make_async_copy(geo_hbm, geo, in_sem.at[0]),
        pltpu.make_async_copy(mass_hbm, mass, in_sem.at[1]),
        pltpu.make_async_copy(load_hbm, load, in_sem.at[2]),
        pltpu.make_async_copy(order_hbm, order, in_sem.at[3]),
    ]

    def peer(stride, width, k):
        digit = lax.rem(me // stride, width)
        return me + (lax.rem(digit + k, width) - digit) * stride

    strides = [int(np.prod(factors[:i])) for i in range(len(factors))]
    blocks = [(stride, square_split(width)) for stride, width in zip(strides, factors)]
    columns_of = [
        (stride * size, width // size) for (stride, size), width in zip(blocks, factors)
    ]

    groups = blocks + columns_of
    relay = blocks[0][1] + 1
    first_chip = me <= 1
    barrier = pltpu.get_barrier_semaphore()

    def signal(semaphore, device):
        pl.semaphore_signal(semaphore, inc=1, device_id=(device,), device_id_type=MESH)

    def greet(semaphore, among, wanted, beside=()):
        for device in beside:
            @pl.when(wanted(device))
            def _():
                signal(semaphore, device)

        for stride, width in among:
            @pl.loop(1, width)
            def _(k):
                device = peer(stride, width, k)

                @pl.when(wanted(device))
                def _():
                    signal(semaphore, device)

    @pl.when(me == count - 1)
    def _():
        signal(barrier, relay)

    @pl.when((me == 1) | (me == relay))
    def _():
        signal(barrier, 0)

    @pl.when((me == 0) | (me == 2))
    def _():
        signal(barrier, 1)

    for copy in fetch[::-1][:1] + fetch[:3]:
        copy.start()
    greet(barrier, groups, lambda device: device > 1, (left, right))

    fetch[3].wait()
    cell = order[...]
    cell8 = jnp.broadcast_to(cell, (points, cols))
    cell_col = jnp.transpose(jnp.broadcast_to(cell.astype(jnp.float32), (cols, cols)))
    lane = lax.broadcasted_iota(jnp.int32, (cols, cols), 1).astype(jnp.float32)
    source = lax.broadcasted_iota(jnp.int32, (cols, cols), 0).astype(jnp.float32)
    inv_row = jnp.sum(jnp.where(cell_col == lane, source, 0.0), axis=0, keepdims=True)
    inv8 = jnp.broadcast_to(inv_row.astype(jnp.int32), (points, cols))
    own_inv[...] = inv8
    pos_z = cell8 % EL_Z
    has_up = cell8 < cols - EL_Z
    has_down = cell8 >= EL_Z
    plus_y = lane_gather(inv8, jnp.where(has_up, cell8 + EL_Z, cell8))
    minus_y = lane_gather(inv8, jnp.where(has_down, cell8 - EL_Z, cell8))
    plus_z = lane_gather(inv8, jnp.where(pos_z == EL_Z - 1, cell8 - (EL_Z - 1), cell8 + 1))
    minus_z = lane_gather(inv8, jnp.where(pos_z == 0, cell8 + (EL_Z - 1), cell8 - 1))

    row_id = lax.broadcasted_iota(jnp.int32, (points, cols), 0)
    for t, table in enumerate((deriv, deriv.T, (deriv * deriv).T)):
        for k in range(points):
            vector = jnp.zeros((points, cols), jnp.float32)
            for m in range(points):
                vector = jnp.where(row_id == m, float(table[m, (m - k) % points]), vector)
            coef[t, k] = vector
    share_z = jnp.where((row_id == 0) | (row_id == points - 1), 0.5, 1.0)
    share_low = jnp.where(has_down, 0.5 * share_z, share_z)
    share_high = jnp.where(has_up, 0.5 * share_z, share_z)

    def share(b):
        return share_low if b == 0 else share_high if b == points - 1 else share_z

    def rotate_contract(value, t):
        total = coef[t, 0] * value
        for k in range(1, points):
            total = total + coef[t, k] * pltpu.roll(value, k, 0)
        return total

    def post(src, dst, send_sem, recv_sem, device):
        pltpu.make_async_remote_copy(
            src_ref=src, dst_ref=dst, send_sem=send_sem, recv_sem=recv_sem,
            device_id=(device,), device_id_type=MESH,
        ).start()

    def settle(ref, send_sem, recv_sem):
        return pltpu.make_async_remote_copy(
            src_ref=ref, dst_ref=ref, send_sem=send_sem, recv_sem=recv_sem,
            device_id=(right,), device_id_type=MESH,
        )

    def line(b):
        return pl.ds(b * points, points)

    def at(base, b):
        if isinstance(base, int):
            return pl.ds(base + b * points, points)
        return pl.ds(pl.multiple_of(base + b * points, points), points)

    def geo_at(k, base, b):
        return at(k * rows + base, b)

    def end_base(s):
        return pl.multiple_of(s * last, points)

    inner = [a * plane for a in range(1, points - 1)]

    def assemble_planes(spots):
        lows = [ref[at(base, 0)] for ref, base in spots]
        highs = [ref[at(base, points - 1)] for ref, base in spots]
        from_low = [lane_gather(low, plus_y) for low in lows]
        from_high = [lane_gather(high, minus_y) for high in highs]
        for i, (ref, base) in enumerate(spots):
            ref[at(base, points - 1)] = highs[i] + jnp.where(has_up, from_low[i], 0.0)
            ref[at(base, 0)] = lows[i] + jnp.where(has_down, from_high[i], 0.0)
        firsts = [pl.ds(base, points, stride=points) for _, base in spots]
        ends_at = [pl.ds(base + points - 1, points, stride=points) for _, base in spots]
        lows = [ref[first] for (ref, _), first in zip(spots, firsts)]
        highs = [ref[end] for (ref, _), end in zip(spots, ends_at)]
        from_low = [lane_gather(low, plus_z) for low in lows]
        from_high = [lane_gather(high, minus_z) for high in highs]
        for i, (ref, _) in enumerate(spots):
            ref[ends_at[i]] = highs[i] + from_low[i]
            ref[firsts[i]] = lows[i] + from_high[i]

    square = deriv * deriv
    fetch[0].wait()
    fetch[1].wait()

    for b in range(points):
        values = [geo[geo_at(0, a * plane, b)] for a in range(points)]
        for a, value in enumerate(contract(values, square.T, True)):
            work[at(a * plane, b)] = value

    def diagonal_plane(base, put):
        values = [geo[geo_at(1, base, b)] for b in range(points)]
        for b, value in enumerate(contract(values, square.T, True)):
            value = value + rotate_contract(geo[geo_at(2, base, b)], 2)
            put(b, value + work[at(base, b)] + mass[at(base, b)])

    for s, base in ((0, 0), (1, last)):

        def put(b, value):
            first_out[s, at(plane, b)] = value

        diagonal_plane(base, put)
    fetch[2].wait()
    for s, base in ((0, 0), (1, last)):
        for b in range(points):
            first_out[s, line(b)] = load[at(base, b)]
    assemble_planes([(first_out.at[s], k * plane) for s in (0, 1) for k in (0, 1)])

    in_block = sum(w - 1 for _, w in blocks)
    in_groups = sum(w - 1 for _, w in groups)
    callers = jnp.where(me == 0, 2, jnp.where(me == 1, 2, 2 + in_groups))
    pl.semaphore_wait(barrier, callers + jnp.where(me == relay, 1, 0))

    def halves_of():
        return [
            (h, pl.ds(k * plane + h * piece, piece)) for h in range(HALVES) for k in (0, 1)
        ]

    def send_first(s, device):
        post(own_inv, near_inv.at[1 - s], sends, first_recv.at[1 - s, 0], device)
        for h, part in halves_of():
            post(
                first_out.at[s, part], first_in.at[1 - s, part], sends,
                first_recv.at[1 - s, h], device,
            )

    def pair_source(s, k):
        return geo.at[pl.ds(pl.multiple_of((k + 1) * rows + s * last, points), plane)]

    def send_pair(s, device):
        for k in (1, 0):
            post(
                pair_source(s, k), pair_in.at[1 - s, k], sends, pair_recv.at[1 - s, k], device
            )

    @pl.when(me == 0)
    def _():
        post(own_inv, relay_inv, sends, relay_recv.at[0], relay)
        for h, part in halves_of():
            post(first_out.at[0, part], relay_first.at[part], sends, relay_recv.at[h], relay)
        for k in (1, 0):
            post(pair_source(0, k), relay_pair.at[k], sends, relay_recv.at[HALVES], relay)

    send_first(near, near_device)

    @pl.when(jnp.logical_not((me == 0) | (me == count - 1) | (me == relay)))
    def _():
        send_first(far, far_device)
        send_pair(far, far_device)

    send_pair(near, near_device)

    @pl.when(jnp.logical_not(first_chip))
    def _():
        greet(ready, blocks, lambda device: device >= 0)
        greet(ready, columns_of, lambda device: device <= 1, (left, right))

    @pl.when(me == relay)
    def _():
        end = count - 1
        for h in range(HALVES):
            landed = geo.at[pl.ds(0, 2 * piece + (0 if h else points))]
            settle(landed, sends, relay_recv.at[h]).wait_recv()
            if h == 0:
                post(relay_inv, near_inv.at[1], sends, first_recv.at[1, 0], end)
            for at_half, part in halves_of():
                if at_half == h:
                    post(
                        relay_first.at[part], first_in.at[1, part], sends,
                        first_recv.at[1, h], end,
                    )
        settle(relay_pair, sends, relay_recv.at[HALVES]).wait_recv()
        for k in (1, 0):
            post(relay_pair.at[k], pair_in.at[1, k], sends, pair_recv.at[1, k], end)

    @pl.when((me == relay))
    def _():
        send_first(far, far_device)
        send_pair(far, far_device)

    for base in inner:
        for b in range(points):
            start[at(base, b)] = load[at(base, b)]

        def put(b, value):
            inverse[at(base, b)] = value

        diagonal_plane(base, put)
    assemble_planes([(ref, base) for base in inner for ref in (start, inverse)])
    for base in inner:
        for b in range(points):
            span = at(base, b)
            scaled = 1.0 / inverse[span]
            inverse[span] = scaled
            vec[span] = scaled * start[span] * (1.0 / spectrum_centre)
    for b in range(points):
        values = [geo[geo_at(0, a * plane, b)] for a in range(points)]
        low, high, both = end_columns(values, deriv)
        for a in range(1, points - 1):
            ends[0, at((a - 1) * plane, b)] = low[a]
            ends[1, at((a - 1) * plane, b)] = high[a]
        cross[line(b)] = both
    assemble_planes(
        [(ends.at[s], base - plane) for s in (0, 1) for base in inner] + [(cross, 0)]
    )

    def inner_to_ends(e, b, values):
        for s in (0, 1):
            inner_part[e, s, line(b)] = sum_of(
                [ends[s, at(base - plane, b)] * v for base, v in zip(inner, values)]
            )

    for b in range(points):
        inner_to_ends(0, b, [vec[at(base, b)] for base in inner])

    @pl.when(me == count - 1)
    def _():
        send_first(far, far_device)
        send_pair(far, far_device)

    @pl.when(me == relay)
    def _():
        settle(relay_along, sends, relay_recv.at[HALVES + 1]).wait_recv()
        post(relay_along, along_in.at[0, 1], sends, along_recv.at[0, 1], count - 1)

    def in_plane(values, slope_geo, flux_geo):
        slopes = contract(values, deriv, False)
        fluxes = [slope_geo(b) * slopes[b] for b in range(points)]
        out = contract(fluxes, deriv.T, False)
        for b in range(points):
            flux = flux_geo(b) * rotate_contract(values[b], 0)
            out[b] = out[b] + rotate_contract(flux, 1)
        return out

    def apply_inner():
        for b in range(points):
            values = [None] + [vec[at(base, b)] for base in inner] + [None]
            slopes = contract(values, deriv, False, skip_in=1)
            fluxes = [geo[geo_at(0, a * plane, b)] * slopes[a] for a in range(points)]
            terms = contract(fluxes, deriv.T, False, skip_out=1)
            for base, value in zip(inner, terms):
                work[at(base, b)] = value
        for base in inner:
            values = [vec[at(base, b)] for b in range(points)]
            terms = in_plane(
                values,
                lambda b: geo[geo_at(1, base, b)],
                lambda b: geo[geo_at(2, base, b)],
            )
            for b in range(points):
                span = at(base, b)
                image[span] = terms[b] + work[span] + mass[span] * values[b]

    apply_inner()
    assemble_planes([(image, base) for base in inner])

    def lines_of(h):
        return range(h * points // HALVES, (h + 1) * points // HALVES)

    def meet(s, h):
        landed = geo.at[pl.ds(0, 2 * piece + (0 if h else points))]
        settle(landed, sends, first_recv.at[s, h]).wait_recv()
        if h == 0:
            across[s] = lane_gather(near_inv[s], cell8)
        columns = across[s]
        base = end_base(s)
        for b in lines_of(h):
            span = at(base, b)
            begin = first_out[s, line(b)] + lane_gather(first_in[s, line(b)], columns)
            whole = first_out[s, at(plane, b)] + lane_gather(first_in[s, at(plane, b)], columns)
            scaled = 1.0 / whole
            face_diag[s, line(b)] = whole
            start[span] = begin
            inverse[span] = scaled
            vec[span] = scaled * begin * (1.0 / spectrum_centre)

    def put_along(e, s, other):
        base = end_base(other)
        for b in range(points):
            along_out[e, s, line(b)] = (
                inner_part[e, s, line(b)] + cross[line(b)] * vec[at(base, b)]
            )

    def post_along(e, s, device):
        post(
            along_out.at[e, s], along_in.at[e, 1 - s], sends,
            along_recv.at[e, 1 - s], device,
        )

    def send_along(e, s, other, device):
        put_along(e, s, other)
        post_along(e, s, device)

    def join_pair(s, k):
        settle(pair_in.at[s, k], sends, pair_recv.at[s, k]).wait_recv()
        columns = across[s]
        for b in range(points):
            own = geo[geo_at(k + 1, s * last, b)]
            pair[s, k, line(b)] = own + lane_gather(pair_in[s, k, line(b)], columns)

    def first_third(s):
        join_pair(s, 1)
        for b in range(points):
            span = at(end_base(s), b)
            both = pair[s, 1, line(b)]
            value = vec[span]
            own = rotate_contract(both, 2)
            pair_diag[s, line(b)] = own
            image[span] = rotate_contract(both * rotate_contract(value, 0), 1) - own * value

    def first_second(s):
        join_pair(s, 0)
        both = [pair[s, 0, line(b)] for b in range(points)]
        values = [vec[at(end_base(s), b)] for b in range(points)]
        own = contract(both, square.T, True)
        slopes = contract(values, deriv, False)
        terms = contract([g * slope for g, slope in zip(both, slopes)], deriv.T, False)
        for b in range(points):
            span = at(end_base(s), b)
            pair_diag[s, line(b)] = pair_diag[s, line(b)] + own[b]
            image[span] = image[span] + terms[b] - own[b] * values[b]
        assemble_planes([(image, end_base(s))])

    def apply_end(s, ref):
        base = end_base(s)
        values = [vec[at(base, b)] for b in range(points)]
        terms = in_plane(values, lambda b: pair[s, 0, line(b)], lambda b: pair[s, 1, line(b)])
        for b in range(points):
            ref[at(base, b)] = terms[b] - pair_diag[s, line(b)] * values[b]

    ratio_sigma = spectrum_centre / spectrum_half
    rho_prev = 1.0 / ratio_sigma
    rho_next = 1.0 / (2.0 * ratio_sigma - rho_prev)
    on_misfit = 2.0 * rho_next / spectrum_half
    on_start = (1.0 + rho_next * rho_prev) / spectrum_centre + on_misfit

    def add_ends(base, b):
        return (
            image[at(base, b)]
            + ends[0, at(base - plane, b)] * vec[at(0, b)]
            + ends[1, at(base - plane, b)] * vec[at(last, b)]
        )

    def join_along(e, s, columns, b):
        span = at(end_base(s), b)
        return (
            image[span] + face_diag[s, line(b)] * vec[span] + along_out[e, s, line(b)]
            + lane_gather(along_in[e, s, line(b)], columns)
        )

    def second_end(s):
        settle(along_in.at[0, s], sends, along_recv.at[0, s]).wait_recv()
        columns = across[s]
        for b in range(points):
            span = at(end_base(s), b)
            total = join_along(0, s, columns, b)
            vec[span] = inverse[span] * (on_start * start[span] - on_misfit * total)

    on_load, products = [], []

    def second_inner(h):
        for b in lines_of(h):
            values = []
            for base in inner:
                span = at(base, b)
                total = add_ends(base, b)
                value = inverse[span] * (on_start * start[span] - on_misfit * total)
                vec[span] = value
                values.append(value)
            inner_to_ends(1, b, values)
            slopes = contract([None] + values + [None], deriv, False, skip_in=1)
            for a, slope in enumerate(slopes):
                products.append(geo[geo_at(0, a * plane, b)] * (slope * slope))
            for base, value in zip(inner, values):
                span = at(base, b)
                turned = rotate_contract(value, 0)
                on_load.append(load[span] * value)
                products.append(
                    geo[geo_at(2, base, b)] * (turned * turned) + mass[span] * (value * value)
                )

    def energy_inner():
        for base in inner:
            slopes = contract([vec[at(base, b)] for b in range(points)], deriv, False)
            for b, slope in enumerate(slopes):
                products.append(geo[geo_at(1, base, b)] * (slope * slope))

    def energy_end(s):
        base = end_base(s)
        values = [vec[at(base, b)] for b in range(points)]
        slopes = contract(values, deriv, False)
        for b, value in enumerate(values):
            turned = rotate_contract(value, 0)
            weighted = share(b) * value
            on_load.append(0.5 * weighted * start[at(base, b)])
            products.append(
                0.5 * (
                    pair[s, 0, line(b)] * (slopes[b] * slopes[b])
                    + pair[s, 1, line(b)] * (turned * turned)
                    - pair_diag[s, line(b)] * (value * value)
                )
                + weighted * (0.5 * face_diag[s, line(b)] * value + 2.0 * inner_part[1, s, line(b)])
            )

    for h in range(HALVES):
        meet(near, h)
    put_along(0, far, near)

    @pl.when(me > 0)
    def _():
        post_along(0, far, far_device)

    @pl.when(me == 0)
    def _():
        post(
            along_out.at[0, 0], relay_along, sends, relay_recv.at[HALVES + 1], relay
        )

    @pl.when(first_chip)
    def _():
        pl.semaphore_wait(ready, in_groups)
        greet(ready, blocks, lambda device: device > 1)
        signal(mate_ready, 1 - me)

    first_third(near)
    first_second(near)
    for h in range(HALVES):
        meet(far, h)
        if h == HALVES - 1:
            send_along(0, near, far, near_device)
        second_inner(h)
    energy_inner()

    @pl.when(first_chip)
    def _():
        pl.semaphore_wait(mate_ready, 1)

    @pl.when(jnp.logical_not(first_chip))
    def _():
        pl.semaphore_wait(ready, in_block)

    first_third(far)

    @pl.when(jnp.logical_not(long_way))
    def _():
        first_second(far)

    early = jnp.where(long_way, near, far)
    late = 1 - early
    early_device = jnp.where(long_way, near_device, far_device)
    late_device = jnp.where(long_way, far_device, near_device)
    second_end(early)
    send_along(1, late, early, late_device)
    energy_end(early)
    on_load[:] = [sum_of(on_load)]
    products[:] = [sum_of(products)]

    @pl.when(long_way)
    def _():
        first_second(far)

    second_end(late)
    energy_end(late)
    for b in range(points):
        products.append(
            2.0 * share(b) * cross[line(b)] * vec[at(0, b)] * vec[at(last, b)]
        )
    total = jnp.concatenate(
        [jnp.sum(sum_of(part), axis=0, keepdims=True) for part in (on_load, products)], axis=1
    )

    def sum_copy(i, k):
        stride, width = strides[i], factors[i]
        return pltpu.make_async_remote_copy(
            src_ref=sums.at[i], dst_ref=parts_in[i].at[k - 1],
            send_sem=sum_send.at[i], recv_sem=sum_recv.at[i],
            device_id=(peer(stride, width, k),), device_id_type=MESH,
        )

    def start_sum(i, value):
        sums[i] = value

        width = factors[i]
        digit = lax.rem(me // strides[i], width)

        @pl.loop(0, width - 1)
        def _(j):
            target = j + jnp.where(j >= digit, 1, 0)
            sum_copy(i, lax.rem(target - digit + width, width)).start()

    def finish_sum(i, value):
        settle(parts_in[i], sum_send.at[i], sum_recv.at[i]).wait()
        return sum_of([value] + [parts_in[i][k] for k in range(factors[i] - 1)])

    start_sum(0, total)
    send_along(1, early, late, early_device)

    apply_inner()
    for s in (near, far):
        apply_end(s, image)
    assemble_planes([(image, base) for base in [0] + inner + [last]])
    for base in inner:
        for b in range(points):
            image[at(base, b)] = add_ends(base, b)
    for s in (near, far):
        settle(along_in.at[1, s], sends, along_recv.at[1, s]).wait_recv()
        columns = across[s]
        for b in range(points):
            image[at(end_base(s), b)] = join_along(1, s, columns, b)
    sent = 12 * plane + 2 * points
    passed_on = 5 * plane + points

    @pl.when(me == relay)
    def _():
        settle(geo.at[pl.ds(0, sent + passed_on)], sends, first_recv.at[0, 0]).wait_send()

    @pl.when(me != relay)
    def _():
        settle(geo.at[pl.ds(0, sent)], sends, first_recv.at[0, 0]).wait_send()

    for i in range(len(factors)):
        if i:
            start_sum(i, total)
        total = finish_sum(i, total)
    numerator = jnp.sum(total[:, :cols], axis=1, keepdims=True)
    denominator = jnp.sum(total[:, cols:], axis=1, keepdims=True)
    size_ref[...] = jnp.broadcast_to(numerator / denominator, (points, cols))


def finish(pieces, points, start, vec, image, size, sol_hbm, res_hbm, sol, res, sems):
    rows, cols = start.shape
    scale = size[...]
    step = rows // pieces
    copies = []
    for i in range(pieces):
        part = pl.ds(i * step, step)
        for j in range(step // points):
            span = pl.ds(i * step + j * points, points)
            sol[span] = scale * vec[span]
            res[span] = start[span] - scale * image[span]
        for k, (src, dst) in enumerate(((sol, sol_hbm), (res, res_hbm))):
            copy = pltpu.make_async_copy(src.at[part], dst.at[part], sems.at[k, i])
            copy.start()
            copies.append(copy)
    for copy in copies:
        copy.wait()


PIECES = 2


def on_device(count, load_terms, geometry, mass_terms, element_order):
    points = load_terms.shape[0]
    cols = load_terms.shape[3]
    plane = points * points
    rows = points * plane
    deriv = gll_derivative(points)
    factors = radices(count)
    f32 = jnp.float32

    def room(*shape, dtype=f32):
        return pltpu.VMEM(shape + (cols,), dtype)

    dma = pltpu.SemaphoreType.DMA
    scratch = (
        [room(rows), room(3 * rows), room(rows), room(rows), room(rows)]
        + [
            room(2, 2 * plane), room(2, 2 * plane), room(2, 2, plane), room(2, 2, plane),
            room(2, plane), room(2, plane),
            room(2, rows - 2 * plane), room(plane), room(2, 2, plane),
            room(2, 2, plane), room(2, 2, plane),
            room(points, dtype=jnp.int32), room(2 * plane), room(2, plane), room(plane),
            room(points, dtype=jnp.int32), room(2, points, dtype=jnp.int32),
            room(2, points, dtype=jnp.int32), room(1, dtype=jnp.int32),
            room(3, points, points),
            pltpu.VMEM((len(factors), 1, 2 * cols), f32),
        ]
        + [pltpu.VMEM((w - 1, 1, 2 * cols), f32) for w in factors]
        + [
            dma((4,)), dma, dma((2, HALVES)), dma((2, 2)), dma((2, 2)),
            dma((len(factors),)), dma((len(factors),)),
            pltpu.SemaphoreType.REGULAR, pltpu.SemaphoreType.REGULAR, dma((HALVES + 2,)),
        ]
    )
    hbm = pl.BlockSpec(memory_space=pl.ANY)
    vmem = pl.BlockSpec(memory_space=pltpu.VMEM)
    pieces = pl.pallas_call(
        functools.partial(kernel, count, points, factors, deriv),
        out_shape=(pltpu.VMEM((rows, cols), f32),) * 3 + (pltpu.VMEM((points, cols), f32),),
        in_specs=[hbm] * 4,
        out_specs=(vmem,) * 4,
        scratch_shapes=scratch,
        compiler_params=pltpu.CompilerParams(collective_id=0, has_side_effects=True),
    )(
        load_terms.reshape(rows, cols),
        geometry.reshape(3 * rows, cols),
        mass_terms.reshape(rows, cols),
        element_order,
    )
    solution_rows, residual_rows = pl.pallas_call(
        functools.partial(finish, PIECES, points),
        out_shape=(jax.ShapeDtypeStruct((rows, cols), f32),) * 2,
        in_specs=[vmem] * 4,
        out_specs=(hbm, hbm),
        scratch_shapes=[room(rows), room(rows), dma((2, PIECES))],
        compiler_params=pltpu.CompilerParams(vmem_limit_bytes=8 * rows * cols * 4),
    )(*pieces)
    shape = load_terms.shape
    return solution_rows.reshape(shape), residual_rows.reshape(shape)


def solution(mesh):
    placed = (
        P(None, None, None, "slab"),
        P(None, None, None, None, "slab"),
        P(None, None, None, "slab"),
        P("slab", None),
    )
    return jax.shard_map(
        functools.partial(on_device, mesh.shape["slab"]),
        mesh=mesh,
        in_specs=placed,
        out_specs=(P(None, None, None, "slab"), P(None, None, None, "slab")),
        check_vma=False,
    )
```
